256 devices in a mesh: gx: 64 (over x, z, core), col: 4 (over y).
Axes of the slice: x: 4, y: 4, z: 8, core: 2. Of those that a mesh axis runs over, the one named last changes fastest.
Arguments:
- grid_field: bfloat16 [64, 256, 256, 128], P('col', 'gx'), may hold values from -6 to 6
- tucker_core: float32 [2, 32, 32, 8, 8, 4], P(None, 'col'), may hold values from -1.5 to 1.5
- in_factor: float32 [64, 32], P('col'), may hold values from -0.75 to 0.75
- out_factor: float32 [64, 32], P('col'), may hold values from -1 to 1
- x_factor: float32 [32, 8], replicated, may hold values from -4 to 4
- y_factor: float32 [32, 8], replicated, may hold values from -4 to 4
- z_factor: float32 [16, 4], replicated, may hold values from -4 to 4
- kx_reach: int32 [32, 16], replicated, may hold values from 1 to 17
Outputs:
- spectral_out: bfloat16 [64, 256, 256, 128], P('col', 'gx')
The draws below stay inside these ranges and needn't reach their ends.
All inputs are finite; a program needn't handle non-finite values.
Results may differ from the reference program's by a relative error of at most 0.001.
Values sent between devices are 32-bit elements; how exact they have to be, the bound alone decides.
No kernel may reach another device: no remote copies, remote signals or barrier semaphores. Data moves between devices by JAX's collectives and lax.ppermute only.
A program may use at most 64 MiB of HBM per device.

```python
import jax
import jax.numpy as jnp
from jax import lax

C = 64
R_IN = 32
R_OUT = 32
RX = 8
RY = 8
RZ = 4
KX = 32
KY = 32
KZ = 16
NY = 256
NZ = 128
NX = 256


def set_ends(result, key, low, top_value):
    dims = result.shape
    spot = [jax.random.randint(jax.random.fold_in(key, axis), (), 0, dims[axis]) for axis in range(len(dims))]
    result = result.at[tuple(spot)].set(low)
    longest = dims.index(max(dims))
    spot[longest] = (spot[longest] + 1) % dims[longest]
    return result.at[tuple(spot)].set(top_value)


def steps_of(key, shape, split, low, top_value):
    loudness, own = 1.0, jax.random.fold_in(key, 6)
    for axis_at, shards_of in split:
        steps = jnp.exp(jax.random.uniform(jax.random.fold_in(own, axis_at), (shards_of,), jnp.float32, low / len(split), top_value / len(split)))
        loudness = loudness * jnp.repeat(steps, shape[axis_at] // shards_of).reshape([-1 if axis == axis_at else 1 for axis in range(len(shape))])
    return loudness


def noise(own_key, extent, scale, reach, pieces=(), kind=jnp.bfloat16):
    values = jax.random.normal(own_key, extent, jnp.float32) * scale
    if len(pieces) > 0:
        values = steps_of(own_key, extent, pieces, -0.22, 0.18) * values
    return jnp.clip(values, min=-reach, max=reach).astype(kind)


def setup_inputs(seed: int = 0) -> dict:
    streams_of = jax.random.split(jax.random.key(seed), 9)
    grid_field = noise(streams_of[0], (C, NX, NY, NZ), 1.0, 6.0, ((0, 4), (1, 64)))
    tucker_core = noise(streams_of[1], (2, R_IN, R_OUT, RX, RY, RZ), (max(1, KX * KY * KZ * R_IN * RX * RY * RZ // (NX * NY * NZ))) ** -0.5, 1.5, ((1, 4),), jnp.float32)
    in_factor = noise(streams_of[2], (C, R_IN), C ** -0.5, 0.75, ((0, 4),), jnp.float32)
    out_factor = noise(streams_of[3], (C, R_OUT), R_OUT ** -0.5, 1.0, ((0, 4),), jnp.float32)
    x_factor = noise(streams_of[4], (KX, RX), 1.0, 4.0, (), jnp.float32)
    y_factor = noise(streams_of[5], (KY, RY), 1.0, 4.0, (), jnp.float32)
    z_factor = noise(streams_of[6], (KZ, RZ), 1.0, 4.0, (), jnp.float32)
    kx_reach = set_ends(jax.random.randint(streams_of[7], (KY, KZ), 1, KX // 2 + 2), jax.random.fold_in(streams_of[7], 1), 1, (KX // 2 + 2) - 1).astype(jnp.int32)
    return {"grid_field": grid_field, "tucker_core": tucker_core, "in_factor": in_factor, "out_factor": out_factor, "x_factor": x_factor, "y_factor": y_factor, "z_factor": z_factor, "kx_reach": kx_reach}


def slot_freq(slot_count):
    slot_index = jnp.arange(slot_count, dtype=jnp.int32)
    return jnp.where(slot_index < slot_count // 2, slot_index, slot_index - slot_count)


def forward_one(channel):
    values = channel.astype(jnp.float32)
    spectrum = jnp.fft.rfft(values, axis=2, norm="ortho")[:, :, :KZ]
    spectrum = jnp.fft.fft(spectrum, axis=1, norm="ortho")
    spectrum = jnp.concatenate([spectrum[:, :KY // 2], spectrum[:, NY - KY // 2:]], axis=1)
    spectrum = jnp.fft.fft(spectrum, axis=0, norm="ortho")
    spectrum = jnp.concatenate([spectrum[:KX // 2], spectrum[NX - KX // 2:]], axis=0)
    return jnp.real(spectrum), jnp.imag(spectrum)


def inverse_one(pair_parts):
    real_part, imag_part = pair_parts
    values = real_part + 1j * imag_part
    zero_fill = jnp.zeros((NX - KX, KY, KZ), values.dtype)
    values = jnp.concatenate([values[:KX // 2], zero_fill, values[KX // 2:]], axis=0)
    values = jnp.fft.ifft(values, axis=0, norm="ortho")
    zero_fill = jnp.zeros((NX, NY - KY, KZ), values.dtype)
    values = jnp.concatenate([values[:, :KY // 2], zero_fill, values[:, KY // 2:]], axis=1)
    values = jnp.fft.ifft(values, axis=1, norm="ortho")
    zero_fill = jnp.zeros((NX, NY, NZ // 2 + 1 - KZ), values.dtype)
    values = jnp.concatenate([values, zero_fill], axis=2)
    return jnp.fft.irfft(values, n=NZ, axis=2, norm="ortho").astype(jnp.bfloat16)


def reference(grid_field, tucker_core, in_factor, out_factor, x_factor, y_factor, z_factor, kx_reach):
    highest = lax.Precision.HIGHEST
    real_spec, imag_spec = lax.map(forward_one, grid_field)
    kept_mask = (jnp.abs(slot_freq(KX))[:, None, None] < kx_reach[None, :, :]).astype(jnp.float32)
    rank_re = jnp.einsum('cr,cijl->rijl', in_factor, real_spec, precision=highest) * kept_mask
    rank_im = jnp.einsum('cr,cijl->rijl', in_factor, imag_spec, precision=highest) * kept_mask

    def per_row(row_items):
        row_re, row_im, y_row = row_items
        partial_value = jnp.einsum('prsabe,b->prsae', tucker_core, y_row, precision=highest)
        kernel = jnp.einsum('prsae,ia,le->prsil', partial_value, x_factor, z_factor, precision=highest)
        mixed_re = (jnp.einsum('rsil,ril->sil', kernel[0], row_re, precision=highest)
                    - jnp.einsum('rsil,ril->sil', kernel[1], row_im, precision=highest))
        mixed_im = (jnp.einsum('rsil,ril->sil', kernel[0], row_im, precision=highest)
                    + jnp.einsum('rsil,ril->sil', kernel[1], row_re, precision=highest))
        out_re = jnp.einsum('os,sil->oil', out_factor, mixed_re, precision=highest)
        out_im = jnp.einsum('os,sil->oil', out_factor, mixed_im, precision=highest)
        return out_re, out_im

    out_re, out_im = lax.map(per_row, (jnp.moveaxis(rank_re, 2, 0), jnp.moveaxis(rank_im, 2, 0), y_factor))
    out_re = jnp.transpose(out_re, (1, 2, 0, 3))
    out_im = jnp.transpose(out_im, (1, 2, 0, 3))
    return lax.map(inverse_one, (out_re, out_im))
```

```python
import functools
import math

import jax
import jax.numpy as jnp
import ml_dtypes
import numpy as np
from jax import lax
from jax.experimental import pallas as pl
from jax.experimental.pallas import tpu as pltpu
from jax.sharding import PartitionSpec as P

F32 = jnp.float32
BF16 = jnp.bfloat16
FREQ_ROWS = 18
ROWS = 40


def halves(table):
    table = table.astype(np.float32)
    high = table.astype(ml_dtypes.bfloat16)
    low = (table - high.astype(np.float32)).astype(ml_dtypes.bfloat16)
    return high, low


def split(values):
    high = values.astype(BF16)
    low = (values - high.astype(F32)).astype(BF16)
    return high, low


def dot(left, right):
    return jnp.dot(left, right, preferred_element_type=F32)


def dot3(left, right):
    lh, ll = split(left)
    rh, rl = split(right)
    return dot(lh, rh) + dot(lh, rl) + dot(ll, rh)


@functools.cache
def y_forward_table():
    y = np.arange(256)[None, :]
    j = np.arange(17)[:, None]
    angle = 2 * np.pi / 256 * (y * j % 256)
    table = np.zeros((ROWS, 256))
    table[:17] = np.cos(angle) / 16
    table[FREQ_ROWS : FREQ_ROWS + 17] = np.sin(angle) / 16
    high, low = halves(table)
    return np.concatenate([high, low], 0)


@functools.cache
def y_inverse_table():
    y = np.arange(256)[:, None]
    j = np.arange(17)[None, :]
    angle = 2 * np.pi / 256 * (y * j % 256)
    table = np.zeros((256, ROWS))
    table[:, :17] = np.cos(angle) / 16
    table[:, FREQ_ROWS : FREQ_ROWS + 17] = -np.sin(angle) / 16
    high, low = halves(table)
    rest = np.zeros((256, 128 - 3 * ROWS), ml_dtypes.bfloat16)
    return np.concatenate([high, low, high, rest], 1)


def z_angles():
    z = np.arange(128)[None, :]
    kz = np.arange(16)[:, None]
    angle = 2 * np.pi / 128 * (z * kz % 128)
    scale = 1 / math.sqrt(128)
    return np.cos(angle) * scale, np.sin(angle) * scale


@functools.cache
def z_forward_table():
    c, s = z_angles()
    table = np.zeros((2, 16, 2, 2, 128))
    for sign_at, sign in ((0, 1.0), (1, -1.0)):
        table[sign_at, :, 0, 0] = c
        table[sign_at, :, 0, 1] = -sign * s
        table[sign_at, :, 1, 0] = -s
        table[sign_at, :, 1, 1] = -sign * c
    high, low = halves(table.reshape(64, 256))
    return np.concatenate([high, low], 0)


@functools.cache
def z_inverse_table():
    c, s = z_angles()
    tables = []
    for pick in range(2):
        table = np.zeros((2, 2, 16, 2, 2, 128))
        for sign_at, sign in ((0, 1.0), (1, -1.0)):
            table[sign_at, pick, :, 0, 0] = c
            table[sign_at, pick, :, 1, 0] = -s
            table[sign_at, pick, :, 0, 1] = sign * s
            table[sign_at, pick, :, 1, 1] = sign * c
        high, low = halves(table.reshape(128, 256))
        tables.append(np.concatenate([high, low, high], 0))
    return np.stack(tables)


def x_angles():
    x = np.arange(256).reshape(64, 4)
    k = np.arange(32)
    freq = np.where(k < 16, k, k - 32)
    angle = 2 * np.pi / 256 * (x[:, :, None] * freq % 256)
    return np.cos(angle) / 16, np.sin(angle) / 16


@functools.cache
def x_forward_table():
    c, s = x_angles()
    table = np.zeros((4, 2, 32, 64, 2))
    table[:, 0, :, :, 0] = c.transpose(1, 2, 0)
    table[:, 0, :, :, 1] = s.transpose(1, 2, 0)
    table[:, 1, :, :, 0] = -s.transpose(1, 2, 0)
    table[:, 1, :, :, 1] = c.transpose(1, 2, 0)
    high, low = halves(table.reshape(256, 128))
    return np.concatenate([high, low, high], 1)


@functools.cache
def x_inverse_table():
    c, s = x_angles()
    table = np.zeros((64, 2, 4, 2, 32))
    table[:, 0, :, 0] = c
    table[:, 0, :, 1] = -s
    table[:, 1, :, 0] = s
    table[:, 1, :, 1] = c
    high, low = halves(table.reshape(128, 256))
    return np.concatenate([high, low, high], 1)


CHUNKS = 8


def forward_kernel(grid_ref, ty_ref, tz_ref, send_ref, stage, lines, arrive):
    count = stage.shape[0]
    per_chunk = count // CHUNKS

    def chunk_copy(n):
        part = pl.ds(n * per_chunk, per_chunk)
        return pltpu.make_async_copy(grid_ref.at[part], stage.at[part], arrive.at[n])

    for n in range(CHUNKS):
        chunk_copy(n).start()
    table = ty_ref[...]
    for n in range(CHUNKS):
        chunk_copy(n).wait()
        for at in range(n * per_chunk, (n + 1) * per_chunk, 2):
            both = jnp.concatenate([stage[at], stage[at + 1]], axis=1)
            out = dot(table, both)
            out = out[:ROWS] + out[ROWS:]
            lines[pl.ds(at, ROWS, stride=count), :] = out[:, :128]
            lines[pl.ds(at + 1, ROWS, stride=count), :] = out[:, 128:]
    tz = tz_ref[...]
    tz_high = tz[:64]
    contract = (((1,), (1,)), ((), ()))
    pieces = []
    for p in range(9):
        at = p * 128
        values = jnp.concatenate(
            [lines[at : at + 128, :], lines[FREQ_ROWS * count + at : FREQ_ROWS * count + at + 128, :]],
            axis=1,
        )
        high, low = split(values)
        first = lax.dot_general(tz, high, contract, preferred_element_type=F32)
        second = lax.dot_general(tz_high, low, contract, preferred_element_type=F32)
        pieces.append(first[:64] + first[64:] + second)
    lane = lax.broadcasted_iota(jnp.int32, (32, 128), 1)
    for p in range(8):
        send_ref[p * 32 : (p + 1) * 32, :] = pieces[p][:32]
        if p > 0:
            send_ref[256 + p * 32 : 256 + (p + 1) * 32, :] = pieces[p][32:]
    send_ref[256:288, :] = jnp.where(lane < 64, pieces[8][32:], pieces[0][32:])


def middle_kernel(
    got_ref, tx_ref, win_ref, scale_ref, core_ref, wout_ref, vx_ref, send_ref
):
    tx = tx_ref[...]
    lane = lax.broadcasted_iota(jnp.int32, (64, 128), 1)
    waves = []
    for pair in range(2):
        cols = [got_ref[(2 * pair + n) * 128 : (2 * pair + n + 1) * 128, :] for n in range(2)]
        high, low = split(jnp.concatenate(cols, axis=1))
        out = dot(tx, jnp.concatenate([high, high, low], axis=0))
        for n in range(2):
            part = out[:, n * 128 : (n + 1) * 128]
            picked = part[:64]
            for x in range(1, 4):
                picked = jnp.where(lane % 4 == x, part[x * 64 : (x + 1) * 64], picked)
            waves.append(picked)
    amplitude = dot3(jnp.concatenate(waves, axis=1), win_ref[...])
    scaled = []
    for h in range(2):
        scale = scale_ref[h]
        scaled.append(amplitude * jnp.concatenate([scale, scale], axis=0))
    left = jnp.concatenate(
        [
            jnp.concatenate([scaled[h][:, m * 128 : (m + 1) * 128] for h in range(2)], axis=1)
            for m in range(2)
        ],
        axis=0,
    )
    core = jnp.concatenate(
        [core_ref[c, a * 8 : (a + 1) * 8, :] for a in range(8) for c in range(4)], axis=0
    )
    mixed = dot3(left, core)
    column = lane[:32] // 32 % 2
    real = jnp.where(column == 0, mixed[0:32], mixed[64:96])
    imag = jnp.where(column == 0, mixed[32:64], mixed[96:128])
    first = lane[:32] < 64
    rows = jnp.concatenate([jnp.where(first, real, imag), jnp.where(first, imag, -real)], axis=0)
    spectra = dot3(rows, wout_ref[...])
    high, low = split(spectra)
    vx = vx_ref[...]
    for pair in range(2):
        sides = []
        for n in range(2):
            at = (2 * pair + n) * 128
            zero = jnp.zeros((64, 128), F32)
            tiles = [
                [
                    jnp.where(lane % 4 == x, values[:, at : at + 128].astype(F32), zero)
                    for x in range(4)
                ]
                for values in (high, low)
            ]
            sides.append(jnp.concatenate(tiles[0] + tiles[0] + tiles[1], axis=0).astype(BF16))
        out = dot(vx, jnp.concatenate(sides, axis=1))
        for n in range(2):
            at = (2 * pair + n) * 128
            send_ref[at : at + 128, :] = out[:, n * 128 : (n + 1) * 128]


def inverse_kernel(got_ref, tz_ref, vy_ref, out_ref, lines, stage, leave):
    count = stage.shape[0]
    per_chunk = count // CHUNKS
    lines[2 * FREQ_ROWS * count :, :] = jnp.zeros(
        ((ROWS - 2 * FREQ_ROWS) * count, 128), F32
    )
    row = lax.broadcasted_iota(jnp.int32, (128, 128), 0)
    lane = lax.broadcasted_iota(jnp.int32, (128, 128), 1)

    def emit(p, values, pick):
        high, low = split(values)
        out = dot(jnp.concatenate([high, high, low], axis=1), tz_ref[pick])
        lines[p * 128 : (p + 1) * 128, :] = out[:, :128]
        at = FREQ_ROWS * count + p * 128
        lines[at : at + 128, :] = out[:, 128:]

    for t in range(4):
        block = jnp.concatenate(
            [got_ref[t * 64 : (t + 1) * 64, :], got_ref[256 + t * 64 : 256 + (t + 1) * 64, :]],
            axis=0,
        )
        turned = block.T
        for pick in range(2):
            if t == 0 and pick == 0:
                emit(0, jnp.where((row < 64) & (lane >= 64), 0.0, turned), 0)
                emit(8, jnp.where((row < 64) & (lane >= 64), turned, 0.0), 0)
            else:
                emit(2 * t + pick, turned, pick)

    def chunk_copy(n):
        part = pl.ds(n * per_chunk, per_chunk)
        return pltpu.make_async_copy(stage.at[part], out_ref.at[part], leave.at[n])

    vy = vy_ref[...]
    for n in range(CHUNKS):
        for at in range(n * per_chunk, (n + 1) * per_chunk, 2):
            both = jnp.concatenate(
                [
                    lines[pl.ds(at, ROWS, stride=count), :],
                    lines[pl.ds(at + 1, ROWS, stride=count), :],
                ],
                axis=1,
            )
            high = both.astype(BF16).astype(F32)
            low = both - high
            rest = jnp.zeros((128 - 3 * ROWS, 256), F32)
            right = jnp.concatenate([high, high, low, rest], axis=0).astype(BF16)
            out = dot(vy, right).astype(BF16)
            stage[at] = out[:, :128]
            stage[at + 1] = out[:, 128:]
        chunk_copy(n).start()
    for n in range(CHUNKS):
        chunk_copy(n).wait()


VMEM = pl.BlockSpec(memory_space=pltpu.VMEM)
ANY = pl.BlockSpec(memory_space=pl.ANY)


def forward_call(grid_field):
    count, grid_y, grid_z = grid_field.shape
    return pl.pallas_call(
        forward_kernel,
        out_shape=jax.ShapeDtypeStruct((512, 128), F32),
        in_specs=[ANY, VMEM, VMEM],
        out_specs=VMEM,
        scratch_shapes=[
            pltpu.VMEM((count, grid_y, grid_z), BF16),
            pltpu.VMEM((ROWS * count, 128), F32),
            pltpu.SemaphoreType.DMA((CHUNKS,)),
        ],
        name="forward_yz",
    )(grid_field, y_forward_table(), z_forward_table())


def middle_call(got, win, scale, core, wout):
    return pl.pallas_call(
        middle_kernel,
        out_shape=jax.ShapeDtypeStruct((512, 128), F32),
        in_specs=[VMEM] * 7,
        out_specs=VMEM,
        name="mix_columns",
    )(got, x_forward_table(), win, scale, core, wout, x_inverse_table())


def inverse_call(got, count, grid_y, grid_z):
    return pl.pallas_call(
        inverse_kernel,
        out_shape=jax.ShapeDtypeStruct((count, grid_y, grid_z), BF16),
        in_specs=[VMEM] * 3,
        out_specs=ANY,
        scratch_shapes=[
            pltpu.VMEM((ROWS * count, 128), F32),
            pltpu.VMEM((count, grid_y, grid_z), BF16),
            pltpu.SemaphoreType.DMA((CHUNKS,)),
        ],
        name="inverse_yz",
    )(got, z_inverse_table(), y_inverse_table())


def in_slot_pairs(table):
    return jnp.concatenate([table[:16], table[16:17], table[31:32], table[17:31][::-1]], axis=0)


def swap_over_col(pieces, axis):
    devices = lax.axis_size(axis)
    here = lax.axis_index(axis)
    arrived = [lax.dynamic_slice_in_dim(pieces, here, 1)]
    for step in range(1, devices):
        ring = [(n, (n + step) % devices) for n in range(devices)]
        leaving = lax.dynamic_slice_in_dim(pieces, (here + step) % devices, 1)
        arrived.append(lax.ppermute(leaving, axis, ring))
    order = [arrived[n] for n in (3, 2, 1, 0, 3, 2, 1)]
    return lax.dynamic_slice_in_dim(jnp.concatenate(order, axis=0), devices - 1 - here, devices)


def weights(core, in_factor, out_factor, x_factor, y_factor, z_factor, kx_reach, gx):
    highest = lax.Precision.HIGHEST
    group = gx // 16
    kz = gx % 16
    y_rows = in_slot_pairs(y_factor).reshape(4, 4, 2, 8)
    y_rows = lax.dynamic_slice_in_dim(y_rows, group, 1, 1)[:, 0]
    z_row = lax.dynamic_slice_in_dim(z_factor, kz, 1)[0]
    pick = y_rows[:, :, :, None] * z_row
    cols = jnp.einsum("prsabe,tmbe->tarpms", core, pick, precision=highest)
    factors = jnp.concatenate([in_factor.reshape(4, 128), out_factor.reshape(4, 128)], axis=0)
    sent = jnp.concatenate(
        [cols.reshape(4, 64, 128), jnp.broadcast_to(factors, (4, 8, 128))], axis=1
    )
    got = swap_over_col(sent, "col")
    in_full = got[:, 64:68].reshape(4, 16, 32)
    out_full = got[:, 68:72].reshape(4, 16, 32)
    same = jnp.eye(2, dtype=F32)
    win = jnp.broadcast_to(
        in_full[:, None, :, None, None, None, :]
        * same[None, :, None, None, :, None, None],
        (4, 2, 16, 4, 2, 4, 32),
    ).reshape(512, 256)
    sign = jnp.array([1.0, -1.0], F32)
    wout = jnp.broadcast_to(
        sign[:, None, None, None, None, None, None]
        * same[None, :, None, None, :, None, None]
        * jnp.transpose(out_full, (2, 0, 1))[None, None, :, :, None, :, None],
        (2, 2, 32, 4, 2, 16, 4),
    ).reshape(128, 512)
    col = lax.axis_index("col")
    reach = in_slot_pairs(kx_reach).reshape(4, 4, 2, 16)
    reach = lax.dynamic_slice(reach, (col, group, 0, kz), (1, 1, 2, 1)).reshape(2)
    slot = jnp.arange(32, dtype=jnp.int32)
    freq = jnp.abs(jnp.where(slot < 16, slot, slot - 32))
    weight = jnp.where(kz == 0, 1.0, 2.0).astype(F32)
    kept = (freq[:, None] < reach[None, :]).astype(F32) * weight
    halves_x = jnp.transpose(x_factor.reshape(32, 2, 4), (1, 0, 2))
    scale = jnp.broadcast_to(
        halves_x[:, :, None, :, None] * kept[None, :, :, None, None], (2, 32, 2, 4, 32)
    ).reshape(2, 32, 256)
    return win, scale, got[:, :64], wout


def everyone(values):
    values = values.reshape(256, 2, 128)
    return lax.all_to_all(values, ("col", "gx"), 0, 0, tiled=True).reshape(512, 128)


def per_device(
    grid_field, tucker_core, in_factor, out_factor, x_factor, y_factor, z_factor, kx_reach
):
    channels, planes, grid_y, grid_z = grid_field.shape
    count = channels * planes
    gx = lax.axis_index("gx")
    sent = forward_call(grid_field.reshape(count, grid_y, grid_z))
    got = everyone(sent)
    win, scale, core, wout = weights(
        tucker_core, in_factor, out_factor, x_factor, y_factor, z_factor, kx_reach, gx
    )
    sent = middle_call(got, win, scale, core, wout)
    got = everyone(sent)
    result = inverse_call(got, count, grid_y, grid_z)
    return result.reshape(channels, planes, grid_y, grid_z)


def solution(mesh):
    return jax.shard_map(
        per_device,
        mesh=mesh,
        in_specs=(
            P("col", "gx", None, None),
            P(None, "col", None, None, None, None),
            P("col", None),
            P("col", None),
            P(),
            P(),
            P(),
            P(),
        ),
        out_specs=P("col", "gx", None, None),
        check_vma=False,
    )
```

```python
import functools
import math

import jax
import jax.numpy as jnp
import ml_dtypes
import numpy as np
from jax import lax
from jax.experimental import pallas as pl
from jax.experimental.pallas import tpu as pltpu
from jax.sharding import PartitionSpec as P

F32 = jnp.float32
BF16 = jnp.bfloat16
FREQ_ROWS = 18
ROWS = 40


def halves(table):
    table = table.astype(np.float32)
    high = table.astype(ml_dtypes.bfloat16)
    low = (table - high.astype(np.float32)).astype(ml_dtypes.bfloat16)
    return high, low


def split(values):
    high = values.astype(BF16)
    low = (values - high.astype(F32)).astype(BF16)
    return high, low


def dot(left, right):
    return jnp.dot(left, right, preferred_element_type=F32)


def dot3(left, right):
    lh, ll = split(left)
    rh, rl = split(right)
    return dot(lh, rh) + dot(lh, rl) + dot(ll, rh)


@functools.cache
def y_forward_table():
    y = np.arange(256)[None, :]
    j = np.arange(17)[:, None]
    angle = 2 * np.pi / 256 * (y * j % 256)
    table = np.zeros((ROWS, 256))
    table[:17] = np.cos(angle) / 16
    table[FREQ_ROWS : FREQ_ROWS + 17] = np.sin(angle) / 16
    high, low = halves(table)
    return np.concatenate([high, low], 0)


@functools.cache
def y_inverse_table():
    y = np.arange(256)[:, None]
    j = np.arange(17)[None, :]
    angle = 2 * np.pi / 256 * (y * j % 256)
    table = np.zeros((256, ROWS))
    table[:, :17] = np.cos(angle) / 16
    table[:, FREQ_ROWS : FREQ_ROWS + 17] = -np.sin(angle) / 16
    high, low = halves(table)
    rest = np.zeros((256, 128 - 3 * ROWS), ml_dtypes.bfloat16)
    return np.concatenate([high, low, high, rest], 1)


def z_angles():
    z = np.arange(128)[None, :]
    kz = np.arange(16)[:, None]
    angle = 2 * np.pi / 128 * (z * kz % 128)
    scale = 1 / math.sqrt(128)
    return np.cos(angle) * scale, np.sin(angle) * scale


@functools.cache
def z_forward_table():
    c, s = z_angles()
    table = np.zeros((2, 16, 2, 2, 128))
    for sign_at, sign in ((0, 1.0), (1, -1.0)):
        table[sign_at, :, 0, 0] = c
        table[sign_at, :, 0, 1] = -sign * s
        table[sign_at, :, 1, 0] = -s
        table[sign_at, :, 1, 1] = -sign * c
    high, low = halves(table.reshape(64, 256))
    return np.concatenate([high, low], 0)


@functools.cache
def z_inverse_table():
    c, s = z_angles()
    tables = []
    for pick in range(2):
        table = np.zeros((2, 2, 16, 2, 2, 128))
        for sign_at, sign in ((0, 1.0), (1, -1.0)):
            table[sign_at, pick, :, 0, 0] = c
            table[sign_at, pick, :, 1, 0] = -s
            table[sign_at, pick, :, 0, 1] = sign * s
            table[sign_at, pick, :, 1, 1] = sign * c
        high, low = halves(table.reshape(128, 256))
        tables.append(np.concatenate([high, low, high], 0))
    return np.stack(tables)


def x_angles():
    x = np.arange(256).reshape(64, 4)
    k = np.arange(32)
    freq = np.where(k < 16, k, k - 32)
    angle = 2 * np.pi / 256 * (x[:, :, None] * freq % 256)
    return np.cos(angle) / 16, np.sin(angle) / 16


@functools.cache
def x_forward_table():
    c, s = x_angles()
    table = np.zeros((4, 2, 32, 64, 2))
    table[:, 0, :, :, 0] = c.transpose(1, 2, 0)
    table[:, 0, :, :, 1] = s.transpose(1, 2, 0)
    table[:, 1, :, :, 0] = -s.transpose(1, 2, 0)
    table[:, 1, :, :, 1] = c.transpose(1, 2, 0)
    high, low = halves(table.reshape(256, 128))
    return np.concatenate([high, low, high], 1)


@functools.cache
def x_inverse_table():
    c, s = x_angles()
    table = np.zeros((64, 2, 4, 2, 32))
    table[:, 0, :, 0] = c
    table[:, 0, :, 1] = -s
    table[:, 1, :, 0] = s
    table[:, 1, :, 1] = c
    high, low = halves(table.reshape(128, 256))
    return np.concatenate([high, low, high], 1)


CHUNKS = 8


def forward_kernel(grid_ref, ty_ref, tz_ref, send_ref, stage, lines, arrive):
    count = stage.shape[0]
    per_chunk = count // CHUNKS

    def chunk_copy(n):
        part = pl.ds(n * per_chunk, per_chunk)
        return pltpu.make_async_copy(grid_ref.at[part], stage.at[part], arrive.at[n])

    for n in range(CHUNKS):
        chunk_copy(n).start()
    table = ty_ref[...]
    for n in range(CHUNKS):
        chunk_copy(n).wait()
        for at in range(n * per_chunk, (n + 1) * per_chunk, 2):
            both = jnp.concatenate([stage[at], stage[at + 1]], axis=1)
            out = dot(table, both)
            out = out[:ROWS] + out[ROWS:]
            lines[pl.ds(at, ROWS, stride=count), :] = out[:, :128]
            lines[pl.ds(at + 1, ROWS, stride=count), :] = out[:, 128:]
    tz = tz_ref[...]
    tz_high = tz[:64]
    contract = (((1,), (1,)), ((), ()))
    pieces = []
    for p in range(9):
        at = p * 128
        values = jnp.concatenate(
            [lines[at : at + 128, :], lines[FREQ_ROWS * count + at : FREQ_ROWS * count + at + 128, :]],
            axis=1,
        )
        high, low = split(values)
        first = lax.dot_general(tz, high, contract, preferred_element_type=F32)
        second = lax.dot_general(tz_high, low, contract, preferred_element_type=F32)
        pieces.append(first[:64] + first[64:] + second)
    lane = lax.broadcasted_iota(jnp.int32, (32, 128), 1)
    for p in range(8):
        send_ref[p * 32 : (p + 1) * 32, :] = pieces[p][:32]
        if p > 0:
            send_ref[256 + p * 32 : 256 + (p + 1) * 32, :] = pieces[p][32:]
    send_ref[256:288, :] = jnp.where(lane < 64, pieces[8][32:], pieces[0][32:])


def middle_kernel(
    got_ref, tx_ref, sum_ref, win_ref, scale_ref, core_ref, wout_ref, spread_ref, vx_ref, send_ref
):
    tx = tx_ref[...]
    lane = lax.broadcasted_iota(jnp.int32, (64, 128), 1)
    waves = []
    for pair in range(2):
        cols = [got_ref[(2 * pair + n) * 128 : (2 * pair + n + 1) * 128, :] for n in range(2)]
        high, low = split(jnp.concatenate(cols, axis=1))
        out = dot(tx, jnp.concatenate([high, high, low], axis=0))
        for n in range(2):
            part = out[:, n * 128 : (n + 1) * 128]
            picked = part[:64]
            for x in range(1, 4):
                picked = jnp.where(lane % 4 == x, part[x * 64 : (x + 1) * 64], picked)
            waves.append(picked)
    high, low = split(jnp.concatenate(waves, axis=1))
    spectrum = dot(jnp.concatenate([high, low], axis=0), sum_ref[...])
    high, low = split(spectrum[:64] + spectrum[64:])
    amplitude = dot(jnp.concatenate([high, low, high], axis=1), win_ref[...])
    scale = scale_ref[...]
    scaled = amplitude * jnp.concatenate([scale, scale], axis=0)
    high, low = split(jnp.concatenate([scaled[:, :256], scaled[:, 256:]], axis=0))
    mixed = dot(jnp.concatenate([high, low, high], axis=1), core_ref[...])
    column = lane[:32] // 32 % 2
    real = jnp.where(column == 0, mixed[0:32], mixed[64:96])
    imag = jnp.where(column == 0, mixed[32:64], mixed[96:128])
    first = lane[:32] < 64
    rows = jnp.concatenate([jnp.where(first, real, imag), jnp.where(first, imag, -real)], axis=0)
    high, low = split(rows)
    contract = (((1,), (1,)), ((), ()))
    spectra = lax.dot_general(
        jnp.concatenate([high, low, high], axis=1),
        wout_ref[...],
        contract,
        preferred_element_type=F32,
    )
    high, low = split(spectra)
    both = dot(jnp.concatenate([high, low], axis=0), spread_ref[...])
    vx = vx_ref[...]
    zero = jnp.zeros((64, 128), F32)
    for pair in range(2):
        sides = []
        for n in range(2):
            at = (2 * pair + n) * 128
            tiles = [
                [jnp.where(lane % 4 == x, values[:, at : at + 128], zero) for x in range(4)]
                for values in (both[:64], both[64:])
            ]
            sides.append(jnp.concatenate(tiles[0] + tiles[0] + tiles[1], axis=0).astype(BF16))
        out = dot(vx, jnp.concatenate(sides, axis=1))
        for n in range(2):
            at = (2 * pair + n) * 128
            send_ref[at : at + 128, :] = out[:, n * 128 : (n + 1) * 128]


@functools.cache
def sum_table():
    table = np.zeros((4, 2, 16, 4, 2, 4, 16))
    for m in range(2):
        for col in range(4):
            for c in range(16):
                table[col, m, c, :, m, col, c] = 1
    return table.reshape(512, 128).astype(ml_dtypes.bfloat16)


@functools.cache
def spread_table():
    table = np.zeros((2, 4, 16, 4, 2, 16, 4))
    for m in range(2):
        for col in range(4):
            for c in range(16):
                table[m, col, c, col, m, c, :] = 1
    return table.reshape(128, 512).astype(ml_dtypes.bfloat16)


@functools.cache
def repeat_tables():
    ranks = np.zeros((128, 32, 8))
    for r in range(32):
        ranks[r, r, :] = 1
    parts = np.zeros((2, 128, 2, 2, 32))
    for m in range(2):
        for s in range(32):
            parts[m, 32 + s, 0, m, s] = 1
            parts[m, 32 + s, 1, m, s] = -1
    table = np.concatenate(
        [ranks.reshape(128, 256), parts[0].reshape(128, 128), parts[1].reshape(128, 128)], 1
    )
    return table.astype(ml_dtypes.bfloat16)


def repeater(rows, lanes, run):
    row = lax.broadcasted_iota(jnp.int32, (rows, lanes), 0)
    lane = lax.broadcasted_iota(jnp.int32, (rows, lanes), 1)
    return (lane // run % rows == row).astype(F32)


def exact_dot(left, right, contract=(1, 0)):
    dims = (((contract[0],), (contract[1],)), ((), ()))
    return lax.dot_general(
        left, right, dims, precision=lax.Precision.HIGHEST, preferred_element_type=F32
    )


def slot_of(block, member):
    p = block - 8
    tail = jnp.where(p == 0, 16 + 15 * member, 32 - 2 * p - member)
    return jnp.where(block < 8, 2 * block + member, tail)


def core_kernel(
    core_ref, y_ref, z_ref, in_ref, out_factor_ref, s0, s1, s2, s3
):
    gx = lax.axis_index("gx")
    col = lax.axis_index("col")
    row = lax.broadcasted_iota(jnp.int32, (8, 32), 0)
    lane = lax.broadcasted_iota(jnp.int32, (8, 32), 1)
    block = ((col + row // 2) % 4) * 4 + gx // 16
    chosen_y = (slot_of(block, row % 2) == lane).astype(F32)
    chosen_z = (lane[:, :16] == gx % 16).astype(F32)
    y_rows = exact_dot(chosen_y, y_ref[...], (1, 1))
    z_rows = exact_dot(chosen_z, z_ref[...], (1, 1))
    pick = exact_dot(y_rows, repeater(8, 256, 4)) * exact_dot(z_rows, repeater(4, 256, 1))
    tall = jnp.concatenate(
        [jnp.broadcast_to(pick[n : n + 1], (8, 256)) for n in range(8)], axis=0
    )
    row = lax.broadcasted_iota(jnp.int32, (64, 256), 0)
    lane = lax.broadcasted_iota(jnp.int32, (64, 256), 1)
    tall = jnp.where(row % 8 == lane // 32, tall, 0.0)
    high, low = split(tall)
    both = jnp.concatenate([high, low], axis=0)
    pad = jnp.zeros((64, 96), F32)
    sends = (s0, s1, s2, s3)
    for r in range(8):
        blocks = []
        for part in range(2):
            at = (part * 8 + r) * 256
            values = core_ref[at : at + 256, :]
            right_high, right_low = split(values)
            out = dot(both, right_high)
            out = out[:64] + out[64:] + dot(high, right_low)
            blocks.append(jnp.concatenate([out, pad], axis=1))
        for t in range(4):
            total = blocks[0][t * 16 : t * 16 + 8]
            for part, member in ((0, 1), (1, 0), (1, 1)):
                at = t * 16 + member * 8
                total = total + pltpu.roll(
                    blocks[part][at : at + 8], 64 * part + 32 * member, 1
                )
            sends[t][r * 8 : (r + 1) * 8, :] = total
    factors = jnp.concatenate(
        [in_ref[...], out_factor_ref[...], jnp.zeros((16, 64), F32)], axis=1
    )
    for t in range(4):
        sends[t][64:80, :] = factors


def weights_kernel(
    p0, p1, p2, p3, x_ref, reach_ref, repeat_ref, win_ref, scale_ref, core_ref, wout_ref, tall
):
    gx = lax.axis_index("gx")
    col = lax.axis_index("col")
    kz = gx % 16
    for t, piece in enumerate((p0, p1, p2, p3)):
        source = (col - t + 4) % 4
        high, low = split(piece[:64, :])
        at = source * 64
        core_ref[pl.ds(pl.multiple_of(at, 64), 64), :] = high
        core_ref[pl.ds(pl.multiple_of(256 + at, 64), 64), :] = high
        core_ref[pl.ds(pl.multiple_of(512 + at, 64), 64), :] = low
        tall[pl.ds(pl.multiple_of(source * 16, 16), 16), :] = piece[64:, :]
    high, low = split(tall[...])
    spread = dot(jnp.concatenate([high, low], axis=0), repeat_ref[...])
    zero = jnp.zeros((64, 256), F32)
    tops = []
    for values in (spread[:64, :256], spread[64:, :256]):
        tops.append(
            jnp.concatenate(
                [jnp.concatenate([values, zero], axis=1), jnp.concatenate([zero, values], axis=1)],
                axis=0,
            ).astype(BF16)
        )
    win_ref[:128] = tops[0]
    win_ref[128:256] = tops[0]
    win_ref[256:] = tops[1]
    outs = [
        jnp.concatenate([values[:, 256:384], values[:, 384:]], axis=0).astype(BF16)
        for values in (spread[:64], spread[64:])
    ]
    wout_ref[...] = jnp.concatenate([outs[0], outs[0], outs[1]], axis=1)
    slot = lax.broadcasted_iota(jnp.int32, (32, 256), 0)
    freq = jnp.where(slot < 16, slot, 32 - slot)
    weight = jnp.where(kz == 0, 1.0, 2.0).astype(F32)
    block = col * 4 + gx // 16
    wide = exact_dot(x_ref[...], repeater(8, 256, 1)) * weight
    for member in range(2):
        reach = reach_ref[kz, slot_of(block, member)]
        scale_ref[:, member * 256 : (member + 1) * 256] = jnp.where(freq < reach, wide, 0.0)


def inverse_kernel(got_ref, tz_ref, vy_ref, out_ref, lines, stage, leave):
    count = stage.shape[0]
    per_chunk = count // CHUNKS
    lines[2 * FREQ_ROWS * count :, :] = jnp.zeros(
        ((ROWS - 2 * FREQ_ROWS) * count, 128), F32
    )
    row = lax.broadcasted_iota(jnp.int32, (128, 128), 0)
    lane = lax.broadcasted_iota(jnp.int32, (128, 128), 1)

    def emit(p, values, pick):
        high, low = split(values)
        out = dot(jnp.concatenate([high, high, low], axis=1), tz_ref[pick])
        lines[p * 128 : (p + 1) * 128, :] = out[:, :128]
        at = FREQ_ROWS * count + p * 128
        lines[at : at + 128, :] = out[:, 128:]

    for t in range(4):
        block = jnp.concatenate(
            [got_ref[t * 64 : (t + 1) * 64, :], got_ref[256 + t * 64 : 256 + (t + 1) * 64, :]],
            axis=0,
        )
        turned = block.T
        for pick in range(2):
            if t == 0 and pick == 0:
                emit(0, jnp.where((row < 64) & (lane >= 64), 0.0, turned), 0)
                emit(8, jnp.where((row < 64) & (lane >= 64), turned, 0.0), 0)
            else:
                emit(2 * t + pick, turned, pick)

    def chunk_copy(n):
        part = pl.ds(n * per_chunk, per_chunk)
        return pltpu.make_async_copy(stage.at[part], out_ref.at[part], leave.at[n])

    vy = vy_ref[...]
    for n in range(CHUNKS):
        for at in range(n * per_chunk, (n + 1) * per_chunk, 2):
            both = jnp.concatenate(
                [
                    lines[pl.ds(at, ROWS, stride=count), :],
                    lines[pl.ds(at + 1, ROWS, stride=count), :],
                ],
                axis=1,
            )
            high = both.astype(BF16).astype(F32)
            low = both - high
            rest = jnp.zeros((128 - 3 * ROWS, 256), F32)
            right = jnp.concatenate([high, high, low, rest], axis=0).astype(BF16)
            out = dot(vy, right).astype(BF16)
            stage[at] = out[:, :128]
            stage[at + 1] = out[:, 128:]
        chunk_copy(n).start()
    for n in range(CHUNKS):
        chunk_copy(n).wait()


VMEM = pl.BlockSpec(memory_space=pltpu.VMEM)


def room(mebibytes):
    return pltpu.CompilerParams(vmem_limit_bytes=mebibytes << 20)


HBM = pl.BlockSpec(memory_space=pltpu.HBM)


def forward_call(grid_field):
    count, grid_y, grid_z = grid_field.shape
    return pl.pallas_call(
        forward_kernel,
        out_shape=pltpu.VMEM((512, 128), F32),
        in_specs=[HBM, VMEM, VMEM],
        out_specs=VMEM,
        scratch_shapes=[
            pltpu.VMEM((count, grid_y, grid_z), BF16),
            pltpu.VMEM((ROWS * count, 128), F32),
            pltpu.SemaphoreType.DMA((CHUNKS,)),
        ],
        name="forward_yz",
    )(grid_field, y_forward_table(), z_forward_table())


def middle_call(got, win, scale, core, wout):
    return pl.pallas_call(
        middle_kernel,
        out_shape=pltpu.VMEM((512, 128), F32),
        in_specs=[VMEM] * 9,
        out_specs=VMEM,
        compiler_params=room(12),
        name="mix_columns",
    )(
        got,
        x_forward_table(),
        sum_table(),
        win,
        scale,
        core,
        wout,
        spread_table(),
        x_inverse_table(),
    )


def core_call(core, y_factor, z_factor, in_factor, out_factor):
    piece = pltpu.VMEM((80, 128), F32)
    return pl.pallas_call(
        core_kernel,
        out_shape=(piece,) * 4,
        in_specs=[VMEM] * 5,
        out_specs=(VMEM,) * 4,
        compiler_params=room(12),
        name="contract_core",
    )(core, y_factor.T, z_factor.T, in_factor, out_factor)


def weights_call(pieces, x_factor, kx_reach):
    return pl.pallas_call(
        weights_kernel,
        out_shape=(
            pltpu.VMEM((384, 512), BF16),
            pltpu.VMEM((32, 512), F32),
            pltpu.VMEM((768, 128), BF16),
            pltpu.VMEM((128, 384), BF16),
        ),
        in_specs=[VMEM] * 5 + [pl.BlockSpec(memory_space=pltpu.SMEM)] + [VMEM],
        out_specs=(VMEM,) * 4,
        scratch_shapes=[pltpu.VMEM((64, 128), F32)],
        compiler_params=room(12),
        name="build_weights",
    )(*pieces, x_factor, kx_reach.T, repeat_tables())


def inverse_call(got, count, grid_y, grid_z):
    return pl.pallas_call(
        inverse_kernel,
        out_shape=pltpu.HBM((count, grid_y, grid_z), BF16),
        in_specs=[VMEM] * 3,
        out_specs=HBM,
        scratch_shapes=[
            pltpu.VMEM((ROWS * count, 128), F32),
            pltpu.VMEM((count, grid_y, grid_z), BF16),
            pltpu.SemaphoreType.DMA((CHUNKS,)),
        ],
        compiler_params=room(16),
        name="inverse_yz",
    )(got, z_inverse_table(), y_inverse_table())


def swap_over_col(pieces):
    devices = lax.axis_size("col")
    arrived = [pieces[0]]
    for step in range(1, devices):
        ring = [(n, (n + step) % devices) for n in range(devices)]
        arrived.append(lax.ppermute(pieces[step], "col", ring))
    return arrived


def everyone(values):
    values = values.reshape(256, 2, 128)
    return lax.all_to_all(values, ("col", "gx"), 0, 0, tiled=True).reshape(512, 128)


def per_device(
    grid_field, tucker_core, in_factor, out_factor, x_factor, y_factor, z_factor, kx_reach
):
    channels, planes, grid_y, grid_z = grid_field.shape
    count = channels * planes
    sent = forward_call(grid_field.reshape(count, grid_y, grid_z))
    got = everyone(sent)
    core = jnp.transpose(tucker_core, (0, 1, 3, 4, 5, 2)).reshape(-1, tucker_core.shape[2])
    pieces = core_call(core, y_factor, z_factor, in_factor, out_factor)
    win, scale, core, wout = weights_call(swap_over_col(pieces), x_factor, kx_reach)
    sent = middle_call(got, win, scale, core, wout)
    got = everyone(sent)
    result = inverse_call(got, count, grid_y, grid_z)
    return result.reshape(channels, planes, grid_y, grid_z)


def solution(mesh):
    return jax.shard_map(
        per_device,
        mesh=mesh,
        in_specs=(
            P("col", "gx", None, None),
            P(None, "col", None, None, None, None),
            P("col", None),
            P("col", None),
            P(),
            P(),
            P(),
            P(),
        ),
        out_specs=P("col", "gx", None, None),
        check_vma=False,
    )
```

```python
import functools
import math

import jax
import jax.numpy as jnp
import ml_dtypes
import numpy as np
from jax import lax
from jax.experimental import pallas as pl
from jax.experimental.pallas import tpu as pltpu
from jax.sharding import PartitionSpec as P

F32 = jnp.float32
BF16 = jnp.bfloat16
FREQ_ROWS = 18
ROWS = 40


def halves(table):
    table = table.astype(np.float32)
    high = table.astype(ml_dtypes.bfloat16)
    low = (table - high.astype(np.float32)).astype(ml_dtypes.bfloat16)
    return high, low


def split(values):
    high = values.astype(BF16)
    low = (values - high.astype(F32)).astype(BF16)
    return high, low


def dot(left, right):
    return jnp.dot(left, right, preferred_element_type=F32)


def dot3(left, right):
    lh, ll = split(left)
    rh, rl = split(right)
    return dot(lh, rh) + dot(lh, rl) + dot(ll, rh)


@functools.cache
def y_forward_table():
    y = np.arange(256)[None, :]
    j = np.arange(17)[:, None]
    angle = 2 * np.pi / 256 * (y * j % 256)
    table = np.zeros((ROWS, 256))
    table[:17] = np.cos(angle) / 16
    table[FREQ_ROWS : FREQ_ROWS + 17] = np.sin(angle) / 16
    high, low = halves(table)
    return np.concatenate([high, low], 0)


@functools.cache
def y_inverse_table():
    y = np.arange(256)[:, None]
    j = np.arange(17)[None, :]
    angle = 2 * np.pi / 256 * (y * j % 256)
    table = np.zeros((256, ROWS))
    table[:, :17] = np.cos(angle) / 16
    table[:, FREQ_ROWS : FREQ_ROWS + 17] = -np.sin(angle) / 16
    high, low = halves(table)
    rest = np.zeros((256, 128 - 3 * ROWS), ml_dtypes.bfloat16)
    return np.concatenate([high, low, high, rest], 1)


def z_angles():
    z = np.arange(128)[None, :]
    kz = np.arange(16)[:, None]
    angle = 2 * np.pi / 128 * (z * kz % 128)
    scale = 1 / math.sqrt(128)
    return np.cos(angle) * scale, np.sin(angle) * scale


@functools.cache
def z_forward_table():
    c, s = z_angles()
    table = np.zeros((2, 16, 2, 2, 128))
    for sign_at, sign in ((0, 1.0), (1, -1.0)):
        table[sign_at, :, 0, 0] = c
        table[sign_at, :, 0, 1] = -sign * s
        table[sign_at, :, 1, 0] = -s
        table[sign_at, :, 1, 1] = -sign * c
    high, low = halves(table.reshape(64, 256))
    return np.concatenate([high, low], 0)


@functools.cache
def z_inverse_table():
    c, s = z_angles()
    tables = []
    for pick in range(2):
        table = np.zeros((2, 2, 16, 2, 2, 128))
        for sign_at, sign in ((0, 1.0), (1, -1.0)):
            table[sign_at, pick, :, 0, 0] = c
            table[sign_at, pick, :, 1, 0] = -s
            table[sign_at, pick, :, 0, 1] = sign * s
            table[sign_at, pick, :, 1, 1] = sign * c
        high, low = halves(table.reshape(128, 256))
        tables.append(np.concatenate([high, low, high], 0))
    return np.stack(tables)


def x_angles():
    x = np.arange(256).reshape(64, 4)
    k = np.arange(32)
    freq = np.where(k < 16, k, k - 32)
    angle = 2 * np.pi / 256 * (x[:, :, None] * freq % 256)
    return np.cos(angle) / 16, np.sin(angle) / 16


@functools.cache
def x_forward_table():
    c, s = x_angles()
    table = np.zeros((4, 2, 32, 64, 2))
    table[:, 0, :, :, 0] = c.transpose(1, 2, 0)
    table[:, 0, :, :, 1] = s.transpose(1, 2, 0)
    table[:, 1, :, :, 0] = -s.transpose(1, 2, 0)
    table[:, 1, :, :, 1] = c.transpose(1, 2, 0)
    high, low = halves(table.reshape(256, 128))
    return np.concatenate([high, low, high], 1)


@functools.cache
def x_inverse_table():
    c, s = x_angles()
    table = np.zeros((64, 2, 4, 2, 32))
    table[:, 0, :, 0] = c
    table[:, 0, :, 1] = -s
    table[:, 1, :, 0] = s
    table[:, 1, :, 1] = c
    high, low = halves(table.reshape(128, 256))
    return np.concatenate([high, low, high], 1)


CHUNKS = 8


def column_picks(y, z, gx, col):
    row = lax.broadcasted_iota(jnp.int32, (8, 32), 0)
    lane = lax.broadcasted_iota(jnp.int32, (8, 32), 1)
    block = ((col + row // 2) % 4) * 4 + gx // 16
    chosen_y = (slot_of(block, row % 2) == lane).astype(F32)
    chosen_z = (lane[:, :16] == gx % 16).astype(F32)
    y_rows = exact_dot(chosen_y, y, (1, 1))
    z_rows = exact_dot(chosen_z, z, (1, 1))
    pick = exact_dot(y_rows, repeater(8, 256, 4)) * exact_dot(z_rows, repeater(4, 256, 1))
    tall = jnp.concatenate(
        [jnp.broadcast_to(pick[n : n + 1], (8, 256)) for n in range(8)], axis=0
    )
    row = lax.broadcasted_iota(jnp.int32, (64, 256), 0)
    lane = lax.broadcasted_iota(jnp.int32, (64, 256), 1)
    return split(jnp.where(row % 8 == lane // 32, tall, 0.0))


def kept_scale(x, reach, gx, col, scale_ref):
    kz = gx % 16
    slot = lax.broadcasted_iota(jnp.int32, (32, 256), 0)
    freq = jnp.where(slot < 16, slot, 32 - slot).astype(F32)
    weight = jnp.where(kz == 0, 1.0, 2.0).astype(F32)
    block = col * 4 + gx // 16
    wide = exact_dot(x, repeater(8, 256, 1), (0, 0)) * weight
    row = lax.broadcasted_iota(jnp.int32, (16, 32), 0)
    lane = lax.broadcasted_iota(jnp.int32, (16, 32), 1)
    for member in range(2):
        here = (row == kz) & (lane == slot_of(block, member))
        bound = jnp.sum(jnp.where(here, reach.astype(F32), 0.0), axis=1, keepdims=True)
        bound = jnp.sum(bound, axis=0, keepdims=True)
        scale_ref[:, member * 256 : (member + 1) * 256] = jnp.where(freq < bound, wide, 0.0)


def contract_core(core, high, low, in_rows, out_rows, sends):
    both = jnp.concatenate([high, low], axis=0)
    pad = jnp.zeros((64, 96), F32)
    for r in range(8):
        blocks = []
        for part in range(2):
            at = (part * 8 + r) * 256
            right_high, right_low = split(core[at : at + 256, :])
            out = dot(both, right_high)
            out = out[:64] + out[64:] + dot(high, right_low)
            blocks.append(jnp.concatenate([out, pad], axis=1))
        for t in range(4):
            total = blocks[0][t * 16 : t * 16 + 8]
            for part, member in ((0, 1), (1, 0), (1, 1)):
                at = t * 16 + member * 8
                total = total + pltpu.roll(
                    blocks[part][at : at + 8], 64 * part + 32 * member, 1
                )
            sends[t, r * 8 : (r + 1) * 8, :] = total
    factors = jnp.concatenate([in_rows, out_rows, jnp.zeros((16, 64), F32)], axis=1)
    for t in range(4):
        sends[t, 64:80, :] = factors


def forward_kernel(
    grid_ref, core_ref, ty_ref, tz_ref, y_ref, z_ref, x_ref, reach_ref, in_ref, out_factor_ref,
    send_ref, s0, s1, s2, s3, scale_ref,
    stage, core, ty, tz, y, z, x, reach, in_rows, out_rows, lines, send, sends, scale,
    arrive, small, leave,
):
    count = stage.shape[0]
    per_chunk = count // CHUNKS
    gx = lax.axis_index("gx")
    col = lax.axis_index("col")

    def chunk_copy(n):
        part = pl.ds(n * per_chunk, per_chunk)
        return pltpu.make_async_copy(grid_ref.at[part], stage.at[part], arrive.at[n])

    pairs = (
        (y_ref, y), (z_ref, z), (x_ref, x), (reach_ref, reach), (in_ref, in_rows),
        (out_factor_ref, out_rows), (core_ref, core), (ty_ref, ty), (tz_ref, tz),
    )
    copies = [
        pltpu.make_async_copy(source, target, small.at[n])
        for n, (source, target) in enumerate(pairs)
    ]
    for copy in copies[:7]:
        copy.start()
    for n in range(CHUNKS):
        chunk_copy(n).start()
        if n == 0:
            for copy in copies[7:]:
                copy.start()
    for copy in copies[:6]:
        copy.wait()
    high, low = column_picks(y[...], z[...], gx, col)
    kept_scale(x[...], reach[...], gx, col, scale)
    copies[6].wait()
    contract_core(core, high, low, in_rows[...], out_rows[...], sends)
    leaving = [pltpu.make_async_copy(scale, scale_ref, leave.at[0])]
    for t, target in enumerate((s0, s1, s2, s3)):
        leaving.append(pltpu.make_async_copy(sends.at[t], target, leave.at[1 + t]))
    for copy in leaving:
        copy.start()
    copies[7].wait()
    copies[8].wait()
    table = ty[...]
    for n in range(CHUNKS):
        chunk_copy(n).wait()
        for at in range(n * per_chunk, (n + 1) * per_chunk, 2):
            both = jnp.concatenate([stage[at], stage[at + 1]], axis=1)
            out = dot(table, both)
            out = out[:ROWS] + out[ROWS:]
            lines[pl.ds(at, ROWS, stride=count), :] = out[:, :128]
            lines[pl.ds(at + 1, ROWS, stride=count), :] = out[:, 128:]
    both_tz = tz[...]
    tz_high = both_tz[:64]
    contract = (((1,), (1,)), ((), ()))

    def piece(p):
        at = p * 128
        values = jnp.concatenate(
            [lines[at : at + 128, :], lines[FREQ_ROWS * count + at : FREQ_ROWS * count + at + 128, :]],
            axis=1,
        )
        high, low = split(values)
        first = lax.dot_general(both_tz, high, contract, preferred_element_type=F32)
        second = lax.dot_general(tz_high, low, contract, preferred_element_type=F32)
        return first[:64] + first[64:] + second

    def ship(n):
        part = pl.ds(n * 128, 128)
        copy = pltpu.make_async_copy(send.at[part], send_ref.at[part], leave.at[5 + n])
        leaving.append(copy)
        copy.start()

    lane = lax.broadcasted_iota(jnp.int32, (32, 128), 1)
    edges = piece(0), piece(8)
    send[0:32, :] = edges[0][:32]
    send[256:288, :] = jnp.where(lane < 64, edges[1][32:], edges[0][32:])
    for p in range(1, 8):
        values = piece(p)
        send[p * 32 : (p + 1) * 32, :] = values[:32]
        send[256 + p * 32 : 256 + (p + 1) * 32, :] = values[32:]
        if p % 4 == 3:
            ship(p // 4)
            ship(2 + p // 4)
    for copy in leaving:
        copy.wait()


def middle_kernel(
    got_ref, tables_ref, win_ref, scale_ref, core_ref, wout_ref, send_ref
):
    tx = table_of(tables_ref, "tx")
    lane = lax.broadcasted_iota(jnp.int32, (64, 128), 1)
    waves = []
    for pair in range(2):
        cols = [got_ref[(2 * pair + n) * 128 : (2 * pair + n + 1) * 128, :] for n in range(2)]
        high, low = split(jnp.concatenate(cols, axis=1))
        out = dot(tx, jnp.concatenate([high, high, low], axis=0))
        for n in range(2):
            part = out[:, n * 128 : (n + 1) * 128]
            picked = part[:64]
            for x in range(1, 4):
                picked = jnp.where(lane % 4 == x, part[x * 64 : (x + 1) * 64], picked)
            waves.append(picked)
    high, low = split(jnp.concatenate(waves, axis=1))
    spectrum = dot(jnp.concatenate([high, low], axis=0), table_of(tables_ref, "sum"))
    high, low = split(spectrum[:64] + spectrum[64:])
    amplitude = dot(jnp.concatenate([high, low, high], axis=1), win_ref[...])
    scale = scale_ref[...]
    scaled = amplitude * jnp.concatenate([scale, scale], axis=0)
    high, low = split(jnp.concatenate([scaled[:, :256], scaled[:, 256:]], axis=0))
    mixed = dot(jnp.concatenate([high, low, high], axis=1), core_ref[...])
    column = lane[:32] // 32 % 2
    real = jnp.where(column == 0, mixed[0:32], mixed[64:96])
    imag = jnp.where(column == 0, mixed[32:64], mixed[96:128])
    first = lane[:32] < 64
    rows = jnp.concatenate([jnp.where(first, real, imag), jnp.where(first, imag, -real)], axis=0)
    high, low = split(rows)
    contract = (((1,), (1,)), ((), ()))
    spectra = lax.dot_general(
        jnp.concatenate([high, low, high], axis=1),
        wout_ref[...],
        contract,
        preferred_element_type=F32,
    )
    high, low = split(spectra)
    both = dot(jnp.concatenate([high, low], axis=0), table_of(tables_ref, "spread"))
    vx = table_of(tables_ref, "vx")
    zero = jnp.zeros((64, 128), F32)
    for pair in range(2):
        sides = []
        for n in range(2):
            at = (2 * pair + n) * 128
            tiles = [
                [jnp.where(lane % 4 == x, values[:, at : at + 128], zero) for x in range(4)]
                for values in (both[:64], both[64:])
            ]
            sides.append(jnp.concatenate(tiles[0] + tiles[0] + tiles[1], axis=0).astype(BF16))
        out = dot(vx, jnp.concatenate(sides, axis=1))
        for n in range(2):
            at = (2 * pair + n) * 128
            send_ref[at : at + 128, :] = out[:, n * 128 : (n + 1) * 128]


@functools.cache
def sum_table():
    table = np.zeros((4, 2, 16, 4, 2, 4, 16))
    for m in range(2):
        for col in range(4):
            for c in range(16):
                table[col, m, c, :, m, col, c] = 1
    return table.reshape(512, 128).astype(ml_dtypes.bfloat16)


@functools.cache
def spread_table():
    table = np.zeros((2, 4, 16, 4, 2, 16, 4))
    for m in range(2):
        for col in range(4):
            for c in range(16):
                table[m, col, c, col, m, c, :] = 1
    return table.reshape(128, 512).astype(ml_dtypes.bfloat16)


@functools.cache
def repeat_tables():
    ranks = np.zeros((128, 32, 8))
    for r in range(32):
        ranks[r, r, :] = 1
    parts = np.zeros((2, 128, 2, 2, 32))
    for m in range(2):
        for s in range(32):
            parts[m, 32 + s, 0, m, s] = 1
            parts[m, 32 + s, 1, m, s] = -1
    table = np.concatenate(
        [ranks.reshape(128, 256), parts[0].reshape(128, 128), parts[1].reshape(128, 128)], 1
    )
    return table.astype(ml_dtypes.bfloat16)


def repeater(rows, lanes, run):
    row = lax.broadcasted_iota(jnp.int32, (rows, lanes), 0)
    lane = lax.broadcasted_iota(jnp.int32, (rows, lanes), 1)
    return (lane // run % rows == row).astype(F32)


def exact_dot(left, right, contract=(1, 0)):
    dims = (((contract[0],), (contract[1],)), ((), ()))
    return lax.dot_general(
        left, right, dims, precision=lax.Precision.HIGHEST, preferred_element_type=F32
    )


def slot_of(block, member):
    p = block - 8
    tail = jnp.where(p == 0, 16 + 15 * member, 32 - 2 * p - member)
    return jnp.where(block < 8, 2 * block + member, tail)


def weights_kernel(p0, p1, p2, p3, tables_ref, win_ref, core_ref, wout_ref, tall):
    col = lax.axis_index("col")
    for t, piece in enumerate((p0, p1, p2, p3)):
        source = (col - t + 4) % 4
        high, low = split(piece[:64, :])
        at = source * 64
        core_ref[pl.ds(pl.multiple_of(at, 64), 64), :] = high
        core_ref[pl.ds(pl.multiple_of(256 + at, 64), 64), :] = high
        core_ref[pl.ds(pl.multiple_of(512 + at, 64), 64), :] = low
        tall[pl.ds(pl.multiple_of(source * 16, 16), 16), :] = piece[64:, :]
    high, low = split(tall[...])
    spread = dot(jnp.concatenate([high, low], axis=0), table_of(tables_ref, "repeat"))
    zero = jnp.zeros((64, 256), F32)
    tops = []
    for values in (spread[:64, :256], spread[64:, :256]):
        tops.append(
            jnp.concatenate(
                [jnp.concatenate([values, zero], axis=1), jnp.concatenate([zero, values], axis=1)],
                axis=0,
            ).astype(BF16)
        )
    win_ref[:128] = tops[0]
    win_ref[128:256] = tops[0]
    win_ref[256:] = tops[1]
    outs = [
        jnp.concatenate([values[:, 256:384], values[:, 384:]], axis=0).astype(BF16)
        for values in (spread[:64], spread[64:])
    ]
    wout_ref[...] = jnp.concatenate([outs[0], outs[0], outs[1]], axis=1)

def inverse_kernel(got_ref, tables_ref, out_ref, lines, stage, leave):
    count = stage.shape[0]
    per_chunk = count // CHUNKS
    lines[2 * FREQ_ROWS * count :, :] = jnp.zeros(
        ((ROWS - 2 * FREQ_ROWS) * count, 128), F32
    )
    tz = [table_of(tables_ref, "tz0"), table_of(tables_ref, "tz1")]
    row = lax.broadcasted_iota(jnp.int32, (128, 128), 0)
    lane = lax.broadcasted_iota(jnp.int32, (128, 128), 1)

    def emit(p, values, pick):
        high, low = split(values)
        out = dot(jnp.concatenate([high, high, low], axis=1), tz[pick])
        lines[p * 128 : (p + 1) * 128, :] = out[:, :128]
        at = FREQ_ROWS * count + p * 128
        lines[at : at + 128, :] = out[:, 128:]

    for t in range(4):
        block = jnp.concatenate(
            [got_ref[t * 64 : (t + 1) * 64, :], got_ref[256 + t * 64 : 256 + (t + 1) * 64, :]],
            axis=0,
        )
        turned = block.T
        for pick in range(2):
            if t == 0 and pick == 0:
                emit(0, jnp.where((row < 64) & (lane >= 64), 0.0, turned), 0)
                emit(8, jnp.where((row < 64) & (lane >= 64), turned, 0.0), 0)
            else:
                emit(2 * t + pick, turned, pick)

    def chunk_copy(n):
        part = pl.ds(n * per_chunk, per_chunk)
        return pltpu.make_async_copy(stage.at[part], out_ref.at[part], leave.at[n])

    vy = table_of(tables_ref, "vy")
    for n in range(CHUNKS):
        for at in range(n * per_chunk, (n + 1) * per_chunk, 2):
            both = jnp.concatenate(
                [
                    lines[pl.ds(at, ROWS, stride=count), :],
                    lines[pl.ds(at + 1, ROWS, stride=count), :],
                ],
                axis=1,
            )
            high = both.astype(BF16).astype(F32)
            low = both - high
            rest = jnp.zeros((128 - 3 * ROWS, 256), F32)
            right = jnp.concatenate([high, high, low, rest], axis=0).astype(BF16)
            out = dot(vy, right).astype(BF16)
            stage[at] = out[:, :128]
            stage[at + 1] = out[:, 128:]
        chunk_copy(n).start()
    for n in range(CHUNKS):
        chunk_copy(n).wait()


def parts_of_tables():
    tz = z_inverse_table()
    return {
        "repeat": repeat_tables(),
        "tx": x_forward_table(),
        "sum": sum_table(),
        "spread": spread_table(),
        "vx": x_inverse_table(),
        "tz0": tz[0],
        "tz1": tz[1],
        "vy": y_inverse_table(),
    }


@functools.cache
def all_tables():
    places, blocks, at = {}, [], 0
    for name, table in parts_of_tables().items():
        places[name] = (at, *table.shape)
        for lane in range(0, table.shape[1], 128):
            blocks.append(table[:, lane : lane + 128])
            at += table.shape[0]
    return places, np.concatenate(blocks, 0)


def table_of(tables_ref, name):
    at, rows, lanes = all_tables()[0][name]
    return jnp.concatenate(
        [tables_ref[at + n * rows : at + (n + 1) * rows, :] for n in range(lanes // 128)], axis=1
    )


VMEM = pl.BlockSpec(memory_space=pltpu.VMEM)
HBM = pl.BlockSpec(memory_space=pltpu.HBM)


def room(mebibytes):
    return pltpu.CompilerParams(vmem_limit_bytes=mebibytes << 20)


def forward_call(grid_field, core, y_factor, z_factor, x_factor, kx_reach, in_factor, out_factor):
    count, grid_y, grid_z = grid_field.shape
    operands = (
        grid_field, core, y_forward_table(), z_forward_table(), y_factor.T, z_factor.T,
        x_factor.T, kx_reach.T, in_factor, out_factor,
    )
    piece = jax.ShapeDtypeStruct((80, 128), F32)
    return pl.pallas_call(
        forward_kernel,
        out_shape=(
            jax.ShapeDtypeStruct((512, 128), F32),
            piece,
            piece,
            piece,
            piece,
            jax.ShapeDtypeStruct((32, 512), F32),
        ),
        in_specs=[HBM] * len(operands),
        out_specs=(HBM,) * 6,
        scratch_shapes=[pltpu.VMEM(value.shape, value.dtype) for value in operands]
        + [
            pltpu.VMEM((ROWS * count, 128), F32),
            pltpu.VMEM((512, 128), F32),
            pltpu.VMEM((4, 80, 128), F32),
            pltpu.VMEM((32, 512), F32),
            pltpu.SemaphoreType.DMA((CHUNKS,)),
            pltpu.SemaphoreType.DMA((9,)),
            pltpu.SemaphoreType.DMA((9,)),
        ],
        name="forward_yz",
    )(*operands)


def middle_call(got, win, scale, core, wout):
    return pl.pallas_call(
        middle_kernel,
        out_shape=jax.ShapeDtypeStruct((512, 128), F32),
        in_specs=[VMEM] * 6,
        out_specs=VMEM,
        compiler_params=room(12),
        name="mix_columns",
    )(got, all_tables()[1], win, scale, core, wout)


def weights_call(pieces):
    return pl.pallas_call(
        weights_kernel,
        out_shape=(
            jax.ShapeDtypeStruct((384, 512), BF16),
            jax.ShapeDtypeStruct((768, 128), BF16),
            jax.ShapeDtypeStruct((128, 384), BF16),
        ),
        in_specs=[VMEM] * 5,
        out_specs=(VMEM,) * 3,
        scratch_shapes=[pltpu.VMEM((64, 128), F32)],
        compiler_params=room(12),
        name="build_weights",
    )(*pieces, all_tables()[1])


def inverse_call(got, count, grid_y, grid_z):
    return pl.pallas_call(
        inverse_kernel,
        out_shape=jax.ShapeDtypeStruct((count, grid_y, grid_z), BF16),
        in_specs=[VMEM] * 2,
        out_specs=HBM,
        scratch_shapes=[
            pltpu.VMEM((ROWS * count, 128), F32),
            pltpu.VMEM((count, grid_y, grid_z), BF16),
            pltpu.SemaphoreType.DMA((CHUNKS,)),
        ],
        compiler_params=room(16),
        name="inverse_yz",
    )(got, all_tables()[1])


def swap_over_col(pieces):
    devices = lax.axis_size("col")
    arrived = [pieces[0]]
    for step in range(1, devices):
        ring = [(n, (n + step) % devices) for n in range(devices)]
        arrived.append(lax.ppermute(pieces[step], "col", ring))
    return arrived


def everyone(values):
    values = values.reshape(256, 2, 128)
    return lax.all_to_all(values, ("col", "gx"), 0, 0, tiled=True).reshape(512, 128)


def per_device(
    grid_field, tucker_core, in_factor, out_factor, x_factor, y_factor, z_factor, kx_reach
):
    channels, planes, grid_y, grid_z = grid_field.shape
    count = channels * planes
    core = jnp.transpose(tucker_core, (0, 1, 3, 4, 5, 2)).reshape(-1, tucker_core.shape[2])
    sent, *pieces, scale = forward_call(
        grid_field.reshape(count, grid_y, grid_z),
        core,
        y_factor,
        z_factor,
        x_factor,
        kx_reach,
        in_factor,
        out_factor,
    )
    got = everyone(sent)
    win, core, wout = weights_call(swap_over_col(pieces))
    sent = middle_call(got, win, scale, core, wout)
    got = everyone(sent)
    result = inverse_call(got, count, grid_y, grid_z)
    return result.reshape(channels, planes, grid_y, grid_z)


def solution(mesh):
    return jax.shard_map(
        per_device,
        mesh=mesh,
        in_specs=(
            P("col", "gx", None, None),
            P(None, "col", None, None, None, None),
            P("col", None),
            P("col", None),
            P(),
            P(),
            P(),
            P(),
        ),
        out_specs=P("col", "gx", None, None),
        check_vma=False,
    )
```

```python
import functools
import math

import jax
import jax.numpy as jnp
import ml_dtypes
import numpy as np
from jax import lax
from jax.experimental import pallas as pl
from jax.experimental.pallas import tpu as pltpu
from jax.sharding import PartitionSpec as P

F32 = jnp.float32
BF16 = jnp.bfloat16
FREQ_ROWS = 18
ROWS = 40
PITCH = 68


def halves(table):
    table = table.astype(np.float32)
    high = table.astype(ml_dtypes.bfloat16)
    low = (table - high.astype(np.float32)).astype(ml_dtypes.bfloat16)
    return high, low


def split(values):
    high = values.astype(BF16)
    low = (values - high.astype(F32)).astype(BF16)
    return high, low


def dot(left, right):
    return jnp.dot(left, right, preferred_element_type=F32)


def dot3(left, right):
    lh, ll = split(left)
    rh, rl = split(right)
    return dot(lh, rh) + dot(lh, rl) + dot(ll, rh)


@functools.cache
def y_forward_table():
    y = np.arange(256)[None, :]
    j = np.arange(17)[:, None]
    angle = 2 * np.pi / 256 * (y * j % 256)
    table = np.zeros((ROWS, 256))
    table[:17] = np.cos(angle) / 16
    table[FREQ_ROWS : FREQ_ROWS + 17] = np.sin(angle) / 16
    high, low = halves(table)
    return np.concatenate([high, low], 0)


@functools.cache
def y_inverse_table():
    y = np.arange(256)[:, None]
    j = np.arange(17)[None, :]
    angle = 2 * np.pi / 256 * (y * j % 256)
    table = np.zeros((256, ROWS))
    table[:, :17] = np.cos(angle) / 16
    table[:, FREQ_ROWS : FREQ_ROWS + 17] = -np.sin(angle) / 16
    high, low = halves(table)
    rest = np.zeros((256, 128 - 3 * ROWS), ml_dtypes.bfloat16)
    return np.concatenate([high, low, high, rest], 1)


def z_angles():
    z = np.arange(128)[None, :]
    kz = np.arange(16)[:, None]
    angle = 2 * np.pi / 128 * (z * kz % 128)
    scale = 1 / math.sqrt(128)
    return np.cos(angle) * scale, np.sin(angle) * scale


@functools.cache
def z_forward_table():
    c, s = z_angles()
    table = np.zeros((2, 16, 2, 2, 128))
    for sign_at, sign in ((0, 1.0), (1, -1.0)):
        table[sign_at, :, 0, 0] = c
        table[sign_at, :, 0, 1] = -sign * s
        table[sign_at, :, 1, 0] = -s
        table[sign_at, :, 1, 1] = -sign * c
    high, low = halves(table.reshape(64, 256))
    return np.concatenate([high, low], 0)


@functools.cache
def z_inverse_table():
    c, s = z_angles()
    tables = []
    for pick in range(2):
        table = np.zeros((2, 2, 16, 2, 2, 128))
        for sign_at, sign in ((0, 1.0), (1, -1.0)):
            table[sign_at, pick, :, 0, 0] = c
            table[sign_at, pick, :, 1, 0] = -s
            table[sign_at, pick, :, 0, 1] = sign * s
            table[sign_at, pick, :, 1, 1] = sign * c
        high, low = halves(table.reshape(128, 256))
        tables.append(np.concatenate([high, low, high], 0))
    return np.stack(tables)


def x_angles():
    x = np.arange(256).reshape(64, 4)
    k = np.arange(32)
    freq = np.where(k < 16, k, k - 32)
    angle = 2 * np.pi / 256 * (x[:, :, None] * freq % 256)
    return np.cos(angle) / 16, np.sin(angle) / 16


@functools.cache
def x_forward_table():
    c, s = x_angles()
    table = np.zeros((4, 2, 32, 64, 2))
    table[:, 0, :, :, 0] = c.transpose(1, 2, 0)
    table[:, 0, :, :, 1] = s.transpose(1, 2, 0)
    table[:, 1, :, :, 0] = -s.transpose(1, 2, 0)
    table[:, 1, :, :, 1] = c.transpose(1, 2, 0)
    high, low = halves(table.reshape(256, 128))
    return np.concatenate([high, low, high], 1)


@functools.cache
def x_inverse_table():
    c, s = x_angles()
    table = np.zeros((64, 2, 4, 2, 32))
    table[:, 0, :, 0] = c
    table[:, 0, :, 1] = -s
    table[:, 1, :, 0] = s
    table[:, 1, :, 1] = c
    high, low = halves(table.reshape(128, 256))
    return np.concatenate([high, low, high], 1)


IN_CHUNKS = 4
OUT_CHUNKS = 8


def column_picks(y, z, gx, col):
    row = lax.broadcasted_iota(jnp.int32, (8, 32), 0)
    lane = lax.broadcasted_iota(jnp.int32, (8, 32), 1)
    block = ((col + row // 2) % 4) * 4 + gx // 16
    chosen_y = (slot_of(block, row % 2) == lane).astype(F32)
    chosen_z = (lane[:, :16] == gx % 16).astype(F32)
    y_rows = exact_dot(chosen_y, y, (1, 1))
    z_rows = exact_dot(chosen_z, z, (1, 1))
    pick = exact_dot(y_rows, repeater(8, 256, 4)) * exact_dot(z_rows, repeater(4, 256, 1))
    tall = jnp.concatenate(
        [jnp.broadcast_to(pick[n : n + 1], (8, 256)) for n in range(8)], axis=0
    )
    row = lax.broadcasted_iota(jnp.int32, (64, 256), 0)
    lane = lax.broadcasted_iota(jnp.int32, (64, 256), 1)
    return split(jnp.where(row % 8 == lane // 32, tall, 0.0))


def kept_scale(x, reach, gx, col, scale_ref):
    kz = gx % 16
    slot = lax.broadcasted_iota(jnp.int32, (32, 256), 0)
    freq = jnp.where(slot < 16, slot, 32 - slot).astype(F32)
    weight = jnp.where(kz == 0, 1.0, 2.0).astype(F32)
    block = col * 4 + gx // 16
    wide = exact_dot(x, repeater(8, 256, 1), (0, 0)) * weight
    row = lax.broadcasted_iota(jnp.int32, (16, 32), 0)
    lane = lax.broadcasted_iota(jnp.int32, (16, 32), 1)
    for member in range(2):
        here = (row == kz) & (lane == slot_of(block, member))
        bound = jnp.sum(jnp.where(here, reach.astype(F32), 0.0), axis=1, keepdims=True)
        bound = jnp.sum(bound, axis=0, keepdims=True)
        kept = jnp.where(freq < bound, wide, 0.0)
        scale_ref[member * 64 : member * 64 + 32, :] = kept[:, :128]
        scale_ref[member * 64 + 32 : member * 64 + 64, :] = kept[:, 128:]


def contract_core(core, high, low, in_rows, out_rows, sends):
    both = jnp.concatenate([high, low], axis=0)
    pad = jnp.zeros((64, 96), F32)
    for r in range(8):
        blocks = []
        for part in range(2):
            at = (part * 8 + r) * 256
            right_high, right_low = split(core[at : at + 256, :])
            out = dot(both, right_high)
            out = out[:64] + out[64:] + dot(high, right_low)
            blocks.append(jnp.concatenate([out, pad], axis=1))
        for t in range(4):
            total = blocks[0][t * 16 : t * 16 + 8]
            for part, member in ((0, 1), (1, 0), (1, 1)):
                at = t * 16 + member * 8
                total = total + pltpu.roll(
                    blocks[part][at : at + 8], 64 * part + 32 * member, 1
                )
            sends[t, r * 8 : (r + 1) * 8, :] = total
    factors = jnp.concatenate([in_rows, out_rows, jnp.zeros((16, 64), F32)], axis=1)
    for t in range(4):
        sends[t, 64:80, :] = factors


def forward_kernel(
    grid_ref, core_ref, ty_ref, tz_ref, y_ref, z_ref, x_ref, reach_ref, in_ref, out_factor_ref,
    send_ref, s0, s1, s2, s3,
    stage, core, ty, tz, y, z, x, reach, in_rows, out_rows, lines, send, sends, scale,
    arrive, small, leave,
):
    count = stage.shape[0]
    per_chunk = count // IN_CHUNKS
    gx = lax.axis_index("gx")
    col = lax.axis_index("col")

    def chunk_copy(n):
        part = pl.ds(n * per_chunk, per_chunk)
        return pltpu.make_async_copy(grid_ref.at[part], stage.at[part], arrive.at[n])

    pairs = (
        (y_ref, y), (z_ref, z), (x_ref, x), (reach_ref, reach), (in_ref, in_rows),
        (out_factor_ref, out_rows), (core_ref, core), (ty_ref, ty), (tz_ref, tz),
    )
    copies = [
        pltpu.make_async_copy(source, target, small.at[n])
        for n, (source, target) in enumerate(pairs)
    ]
    for copy in copies[:6]:
        copy.start()
    chunk_copy(0).start()
    for copy in copies[7:]:
        copy.start()
    for n in range(1, IN_CHUNKS):
        chunk_copy(n).start()
    copies[6].start()
    leaving = []
    for copy in copies[:6]:
        copy.wait()
    high, low = column_picks(y[...], z[...], gx, col)
    kept_scale(x[...], reach[...], gx, col, scale)
    copies[7].wait()
    copies[8].wait()
    table = ty[...]
    for n in range(IN_CHUNKS):
        chunk_copy(n).wait()
        for at in range(n * per_chunk, (n + 1) * per_chunk, 2):
            both = jnp.concatenate([stage[at], stage[at + 1]], axis=1)
            out = dot(table, both)
            out = out[:ROWS] + out[ROWS:]
            lines[pl.ds(at, ROWS, stride=PITCH), :] = out[:, :128]
            lines[pl.ds(at + 1, ROWS, stride=PITCH), :] = out[:, 128:]
    both_tz = tz[...]
    tz_high = both_tz[:64]
    contract = (((1,), (1,)), ((), ()))

    def piece(p):
        values = jnp.concatenate(
            [
                jnp.concatenate(
                    [lines[(at + n) * PITCH : (at + n) * PITCH + count, :] for n in range(2)], axis=0
                )
                for at in (2 * p, FREQ_ROWS + 2 * p)
            ],
            axis=1,
        )
        high, low = split(values)
        first = lax.dot_general(both_tz, high, contract, preferred_element_type=F32)
        second = lax.dot_general(tz_high, low, contract, preferred_element_type=F32)
        return first[:64] + first[64:] + second

    def ship(n):
        part = pl.ds(n * 128, 128)
        copy = pltpu.make_async_copy(send.at[part], send_ref.at[part], leave.at[5 + n])
        leaving.append(copy)
        copy.start()

    lane = lax.broadcasted_iota(jnp.int32, (32, 128), 1)
    edges = piece(0), piece(8)
    send[0:32, :] = edges[0][:32]
    send[256:288, :] = jnp.where(lane < 64, edges[1][32:], edges[0][32:])
    for p in range(1, 8):
        values = piece(p)
        send[p * 32 : (p + 1) * 32, :] = values[:32]
        send[256 + p * 32 : 256 + (p + 1) * 32, :] = values[32:]
        if p % 4 == 3:
            ship(p // 4)
            ship(2 + p // 4)
    copies[6].wait()
    contract_core(core, high, low, in_rows[...], out_rows[...], sends)
    last = [pltpu.make_async_copy(scale, s0.at[pl.ds(80, 128)], leave.at[0])]
    for t, target in enumerate((s0.at[pl.ds(0, 80)], s1, s2, s3)):
        last.append(pltpu.make_async_copy(sends.at[t], target, leave.at[1 + t]))
    for copy in last:
        copy.start()
    for copy in leaving + last:
        copy.wait()


def middle_kernel(
    got_ref, tables_ref, win_ref, scale_ref, core_ref, wout_ref, send_ref
):
    tx = table_of(tables_ref, "tx")
    lane = lax.broadcasted_iota(jnp.int32, (64, 128), 1)
    waves = []
    for pair in range(2):
        cols = [got_ref[(2 * pair + n) * 128 : (2 * pair + n + 1) * 128, :] for n in range(2)]
        high, low = split(jnp.concatenate(cols, axis=1))
        out = dot(tx, jnp.concatenate([high, high, low], axis=0))
        for n in range(2):
            part = out[:, n * 128 : (n + 1) * 128]
            picked = part[:64]
            for x in range(1, 4):
                picked = jnp.where(lane % 4 == x, part[x * 64 : (x + 1) * 64], picked)
            waves.append(picked)
    high, low = split(jnp.concatenate(waves, axis=1))
    spectrum = dot(jnp.concatenate([high, low], axis=0), table_of(tables_ref, "sum"))
    high, low = split(spectrum[:64] + spectrum[64:])
    amplitude = dot(jnp.concatenate([high, low, high], axis=1), win_ref[...])
    scale = scale_ref[...]
    scaled = amplitude * jnp.concatenate([scale, scale], axis=0)
    high, low = split(jnp.concatenate([scaled[:, :256], scaled[:, 256:]], axis=0))
    mixed = dot(jnp.concatenate([high, low, high], axis=1), core_ref[...])
    column = lane[:32] // 32 % 2
    real = jnp.where(column == 0, mixed[0:32], mixed[64:96])
    imag = jnp.where(column == 0, mixed[32:64], mixed[96:128])
    first = lane[:32] < 64
    rows = jnp.concatenate([jnp.where(first, real, imag), jnp.where(first, imag, -real)], axis=0)
    high, low = split(rows)
    contract = (((1,), (1,)), ((), ()))
    spectra = lax.dot_general(
        jnp.concatenate([high, low, high], axis=1),
        wout_ref[...],
        contract,
        preferred_element_type=F32,
    )
    high, low = split(spectra)
    both = dot(jnp.concatenate([high, low], axis=0), table_of(tables_ref, "spread"))
    vx = table_of(tables_ref, "vx")
    zero = jnp.zeros((64, 128), F32)
    for pair in range(2):
        sides = []
        for n in range(2):
            at = (2 * pair + n) * 128
            tiles = [
                [jnp.where(lane % 4 == x, values[:, at : at + 128], zero) for x in range(4)]
                for values in (both[:64], both[64:])
            ]
            sides.append(jnp.concatenate(tiles[0] + tiles[0] + tiles[1], axis=0).astype(BF16))
        out = dot(vx, jnp.concatenate(sides, axis=1))
        for n in range(2):
            at = (2 * pair + n) * 128
            send_ref[at : at + 128, :] = out[:, n * 128 : (n + 1) * 128]


@functools.cache
def sum_table():
    table = np.zeros((4, 2, 16, 4, 2, 4, 16))
    for m in range(2):
        for col in range(4):
            for c in range(16):
                table[col, m, c, :, m, col, c] = 1
    return table.reshape(512, 128).astype(ml_dtypes.bfloat16)


@functools.cache
def spread_table():
    table = np.zeros((2, 4, 16, 4, 2, 16, 4))
    for m in range(2):
        for col in range(4):
            for c in range(16):
                table[m, col, c, col, m, c, :] = 1
    return table.reshape(128, 512).astype(ml_dtypes.bfloat16)


@functools.cache
def repeat_tables():
    ranks = np.zeros((128, 32, 8))
    for r in range(32):
        ranks[r, r, :] = 1
    parts = np.zeros((2, 128, 2, 2, 32))
    for m in range(2):
        for s in range(32):
            parts[m, 32 + s, 0, m, s] = 1
            parts[m, 32 + s, 1, m, s] = -1
    table = np.concatenate(
        [ranks.reshape(128, 256), parts[0].reshape(128, 128), parts[1].reshape(128, 128)], 1
    )
    return table.astype(ml_dtypes.bfloat16)


def repeater(rows, lanes, run):
    row = lax.broadcasted_iota(jnp.int32, (rows, lanes), 0)
    lane = lax.broadcasted_iota(jnp.int32, (rows, lanes), 1)
    return (lane // run % rows == row).astype(F32)


def exact_dot(left, right, contract=(1, 0)):
    dims = (((contract[0],), (contract[1],)), ((), ()))
    return lax.dot_general(
        left, right, dims, precision=lax.Precision.HIGHEST, preferred_element_type=F32
    )


def slot_of(block, member):
    p = block - 8
    tail = jnp.where(p == 0, 16 + 15 * member, 32 - 2 * p - member)
    return jnp.where(block < 8, 2 * block + member, tail)


def weights_kernel(
    p0, p1, p2, p3, tables_ref, win_ref, scale_ref, core_ref, wout_ref, tall
):
    col = lax.axis_index("col")
    for n in range(4):
        scale_ref[:, n * 128 : (n + 1) * 128] = p0[80 + n * 32 : 112 + n * 32, :]
    for t, piece in enumerate((p0, p1, p2, p3)):
        source = (col - t + 4) % 4
        high, low = split(piece[:64, :])
        at = source * 64
        core_ref[pl.ds(pl.multiple_of(at, 64), 64), :] = high
        core_ref[pl.ds(pl.multiple_of(256 + at, 64), 64), :] = high
        core_ref[pl.ds(pl.multiple_of(512 + at, 64), 64), :] = low
        tall[pl.ds(pl.multiple_of(source * 16, 16), 16), :] = piece[64:80, :]
    high, low = split(tall[...])
    spread = dot(jnp.concatenate([high, low], axis=0), table_of(tables_ref, "repeat"))
    zero = jnp.zeros((64, 256), F32)
    tops = []
    for values in (spread[:64, :256], spread[64:, :256]):
        tops.append(
            jnp.concatenate(
                [jnp.concatenate([values, zero], axis=1), jnp.concatenate([zero, values], axis=1)],
                axis=0,
            ).astype(BF16)
        )
    win_ref[:128] = tops[0]
    win_ref[128:256] = tops[0]
    win_ref[256:] = tops[1]
    outs = [
        jnp.concatenate([values[:, 256:384], values[:, 384:]], axis=0).astype(BF16)
        for values in (spread[:64], spread[64:])
    ]
    wout_ref[...] = jnp.concatenate([outs[0], outs[0], outs[1]], axis=1)

def inverse_kernel(got_ref, tables_ref, out_ref, lines, stage, leave):
    count = stage.shape[0]
    per_chunk = count // OUT_CHUNKS
    for n in range(2 * FREQ_ROWS, ROWS):
        lines[n * PITCH : n * PITCH + count, :] = jnp.zeros((count, 128), F32)
    tz = [table_of(tables_ref, "tz0"), table_of(tables_ref, "tz1")]
    row = lax.broadcasted_iota(jnp.int32, (128, 128), 0)
    lane = lax.broadcasted_iota(jnp.int32, (128, 128), 1)

    def emit(p, values, pick):
        high, low = split(values)
        out = dot(jnp.concatenate([high, high, low], axis=1), tz[pick])
        for n in range(2):
            rows = out[n * count : (n + 1) * count]
            for first, values in ((2 * p, rows[:, :128]), (FREQ_ROWS + 2 * p, rows[:, 128:])):
                at = (first + n) * PITCH
                lines[at : at + count, :] = values

    for t in range(4):
        block = jnp.concatenate(
            [got_ref[t * 64 : (t + 1) * 64, :], got_ref[256 + t * 64 : 256 + (t + 1) * 64, :]],
            axis=0,
        )
        turned = block.T
        for pick in range(2):
            if t == 0 and pick == 0:
                emit(0, jnp.where((row < 64) & (lane >= 64), 0.0, turned), 0)
                emit(8, jnp.where((row < 64) & (lane >= 64), turned, 0.0), 0)
            else:
                emit(2 * t + pick, turned, pick)

    def chunk_copy(n):
        part = pl.ds(n * per_chunk, per_chunk)
        return pltpu.make_async_copy(stage.at[part], out_ref.at[part], leave.at[n])

    vy = table_of(tables_ref, "vy")
    for n in range(OUT_CHUNKS):
        for at in range(n * per_chunk, (n + 1) * per_chunk, 2):
            both = jnp.concatenate(
                [
                    lines[pl.ds(at, ROWS, stride=PITCH), :],
                    lines[pl.ds(at + 1, ROWS, stride=PITCH), :],
                ],
                axis=1,
            )
            high = both.astype(BF16).astype(F32)
            low = both - high
            rest = jnp.zeros((128 - 3 * ROWS, 256), F32)
            right = jnp.concatenate([high, high, low, rest], axis=0).astype(BF16)
            out = dot(vy, right).astype(BF16)
            stage[at] = out[:, :128]
            stage[at + 1] = out[:, 128:]
        chunk_copy(n).start()
    for n in range(OUT_CHUNKS):
        chunk_copy(n).wait()


def parts_of_tables():
    tz = z_inverse_table()
    return {
        "repeat": repeat_tables(),
        "tx": x_forward_table(),
        "sum": sum_table(),
        "spread": spread_table(),
        "vx": x_inverse_table(),
        "tz0": tz[0],
        "tz1": tz[1],
        "vy": y_inverse_table(),
    }


@functools.cache
def all_tables():
    places, blocks, at = {}, [], 0
    for name, table in parts_of_tables().items():
        places[name] = (at, *table.shape)
        for lane in range(0, table.shape[1], 128):
            blocks.append(table[:, lane : lane + 128])
            at += table.shape[0]
    return places, np.concatenate(blocks, 0)


def table_of(tables_ref, name):
    at, rows, lanes = all_tables()[0][name]
    return jnp.concatenate(
        [tables_ref[at + n * rows : at + (n + 1) * rows, :] for n in range(lanes // 128)], axis=1
    )


VMEM = pl.BlockSpec(memory_space=pltpu.VMEM)
HBM = pl.BlockSpec(memory_space=pltpu.HBM)


def room(mebibytes):
    return pltpu.CompilerParams(vmem_limit_bytes=mebibytes << 20)


def forward_call(grid_field, core, y_factor, z_factor, x_factor, kx_reach, in_factor, out_factor):
    count, grid_y, grid_z = grid_field.shape
    operands = (
        grid_field, core, y_forward_table(), z_forward_table(), y_factor.T, z_factor.T,
        x_factor.T, kx_reach.T, in_factor, out_factor,
    )
    piece = jax.ShapeDtypeStruct((80, 128), F32)
    return pl.pallas_call(
        forward_kernel,
        out_shape=(
            jax.ShapeDtypeStruct((512, 128), F32),
            jax.ShapeDtypeStruct((208, 128), F32),
            piece,
            piece,
            piece,
        ),
        in_specs=[HBM] * len(operands),
        out_specs=(HBM,) * 5,
        scratch_shapes=[pltpu.VMEM(value.shape, value.dtype) for value in operands]
        + [
            pltpu.VMEM((ROWS * PITCH, 128), F32),
            pltpu.VMEM((512, 128), F32),
            pltpu.VMEM((4, 80, 128), F32),
            pltpu.VMEM((128, 128), F32),
            pltpu.SemaphoreType.DMA((IN_CHUNKS,)),
            pltpu.SemaphoreType.DMA((9,)),
            pltpu.SemaphoreType.DMA((9,)),
        ],
        name="forward_yz",
    )(*operands)


def middle_call(got, win, scale, core, wout):
    return pl.pallas_call(
        middle_kernel,
        out_shape=jax.ShapeDtypeStruct((512, 128), F32),
        in_specs=[VMEM] * 6,
        out_specs=VMEM,
        compiler_params=room(12),
        name="mix_columns",
    )(got, all_tables()[1], win, scale, core, wout)


def weights_call(pieces):
    return pl.pallas_call(
        weights_kernel,
        out_shape=(
            jax.ShapeDtypeStruct((384, 512), BF16),
            jax.ShapeDtypeStruct((32, 512), F32),
            jax.ShapeDtypeStruct((768, 128), BF16),
            jax.ShapeDtypeStruct((128, 384), BF16),
        ),
        in_specs=[VMEM] * 5,
        out_specs=(VMEM,) * 4,
        scratch_shapes=[pltpu.VMEM((64, 128), F32)],
        compiler_params=room(12),
        name="build_weights",
    )(*pieces, all_tables()[1])


def inverse_call(got, count, grid_y, grid_z):
    return pl.pallas_call(
        inverse_kernel,
        out_shape=jax.ShapeDtypeStruct((count, grid_y, grid_z), BF16),
        in_specs=[VMEM] * 2,
        out_specs=HBM,
        scratch_shapes=[
            pltpu.VMEM((ROWS * PITCH, 128), F32),
            pltpu.VMEM((count, grid_y, grid_z), BF16),
            pltpu.SemaphoreType.DMA((OUT_CHUNKS,)),
        ],
        compiler_params=room(16),
        name="inverse_yz",
    )(got, all_tables()[1])


def swap_over_col(pieces):
    devices = lax.axis_size("col")
    arrived = [pieces[0]]
    for step in range(1, devices):
        ring = [(n, (n + step) % devices) for n in range(devices)]
        arrived.append(lax.ppermute(pieces[step], "col", ring))
    return arrived


def everyone(values):
    values = values.reshape(256, 2, 128)
    return lax.all_to_all(values, ("col", "gx"), 0, 0, tiled=True).reshape(512, 128)


def per_device(
    grid_field, tucker_core, in_factor, out_factor, x_factor, y_factor, z_factor, kx_reach
):
    channels, planes, grid_y, grid_z = grid_field.shape
    count = channels * planes
    core = jnp.transpose(tucker_core, (0, 1, 3, 4, 5, 2)).reshape(-1, tucker_core.shape[2])
    sent, *pieces = forward_call(
        grid_field.reshape(count, grid_y, grid_z),
        core,
        y_factor,
        z_factor,
        x_factor,
        kx_reach,
        in_factor,
        out_factor,
    )
    got = everyone(sent)
    win, scale, core, wout = weights_call(swap_over_col(pieces))
    sent = middle_call(got, win, scale, core, wout)
    got = everyone(sent)
    result = inverse_call(got, count, grid_y, grid_z)
    return result.reshape(channels, planes, grid_y, grid_z)


def solution(mesh):
    return jax.shard_map(
        per_device,
        mesh=mesh,
        in_specs=(
            P("col", "gx", None, None),
            P(None, "col", None, None, None, None),
            P("col", None),
            P("col", None),
            P(),
            P(),
            P(),
            P(),
        ),
        out_specs=P("col", "gx", None, None),
        check_vma=False,
    )
```

```python
import functools
import math

import jax
import jax.numpy as jnp
import ml_dtypes
import numpy as np
from jax import lax
from jax.experimental import pallas as pl
from jax.experimental.pallas import tpu as pltpu
from jax.sharding import PartitionSpec as P

F32 = jnp.float32
BF16 = jnp.bfloat16
FREQ_ROWS = 18
ROWS = 40
PITCH = 68


def halves(table):
    table = table.astype(np.float32)
    high = table.astype(ml_dtypes.bfloat16)
    low = (table - high.astype(np.float32)).astype(ml_dtypes.bfloat16)
    return high, low


def split(values):
    high = values.astype(BF16)
    low = (values - high.astype(F32)).astype(BF16)
    return high, low


def dot(left, right):
    return jnp.dot(left, right, preferred_element_type=F32)


def dot3(left, right):
    lh, ll = split(left)
    rh, rl = split(right)
    return dot(lh, rh) + dot(lh, rl) + dot(ll, rh)


@functools.cache
def y_forward_table():
    y = np.arange(256)[None, :]
    j = np.arange(17)[:, None]
    angle = 2 * np.pi / 256 * (y * j % 256)
    table = np.zeros((ROWS, 256))
    table[:17] = np.cos(angle) / 16
    table[FREQ_ROWS : FREQ_ROWS + 17] = np.sin(angle) / 16
    high, low = halves(table)
    return np.concatenate([high, low], 0)


@functools.cache
def y_inverse_table():
    y = np.arange(256)[:, None]
    j = np.arange(17)[None, :]
    angle = 2 * np.pi / 256 * (y * j % 256)
    table = np.zeros((256, ROWS))
    table[:, :17] = np.cos(angle) / 16
    table[:, FREQ_ROWS : FREQ_ROWS + 17] = -np.sin(angle) / 16
    high, low = halves(table)
    rest = np.zeros((256, 128 - 3 * ROWS), ml_dtypes.bfloat16)
    return np.concatenate([high, low, high, rest], 1)


def z_angles():
    z = np.arange(128)[None, :]
    kz = np.arange(16)[:, None]
    angle = 2 * np.pi / 128 * (z * kz % 128)
    scale = 1 / math.sqrt(128)
    return np.cos(angle) * scale, np.sin(angle) * scale


@functools.cache
def z_forward_table():
    c, s = z_angles()
    table = np.zeros((2, 16, 2, 2, 128))
    for sign_at, sign in ((0, 1.0), (1, -1.0)):
        table[sign_at, :, 0, 0] = c
        table[sign_at, :, 0, 1] = -sign * s
        table[sign_at, :, 1, 0] = -s
        table[sign_at, :, 1, 1] = -sign * c
    high, low = halves(table.reshape(64, 256))
    return np.concatenate([high, low], 0)


@functools.cache
def z_inverse_table():
    c, s = z_angles()
    tables = []
    for pick in range(2):
        table = np.zeros((2, 2, 16, 2, 2, 128))
        for sign_at, sign in ((0, 1.0), (1, -1.0)):
            table[sign_at, pick, :, 0, 0] = c
            table[sign_at, pick, :, 1, 0] = -s
            table[sign_at, pick, :, 0, 1] = sign * s
            table[sign_at, pick, :, 1, 1] = sign * c
        high, low = halves(table.reshape(128, 256))
        tables.append(np.concatenate([high, low, high], 0))
    return np.stack(tables)


def x_angles():
    x = np.arange(256).reshape(64, 4)
    k = np.arange(32)
    freq = np.where(k < 16, k, k - 32)
    angle = 2 * np.pi / 256 * (x[:, :, None] * freq % 256)
    return np.cos(angle) / 16, np.sin(angle) / 16


@functools.cache
def x_forward_table():
    c, s = x_angles()
    table = np.zeros((4, 2, 32, 64, 2))
    table[:, 0, :, :, 0] = c.transpose(1, 2, 0)
    table[:, 0, :, :, 1] = s.transpose(1, 2, 0)
    table[:, 1, :, :, 0] = -s.transpose(1, 2, 0)
    table[:, 1, :, :, 1] = c.transpose(1, 2, 0)
    high, low = halves(table.reshape(256, 128))
    return np.concatenate([high, low, high], 1)


@functools.cache
def x_inverse_table():
    c, s = x_angles()
    table = np.zeros((64, 2, 4, 2, 32))
    table[:, 0, :, 0] = c
    table[:, 0, :, 1] = -s
    table[:, 1, :, 0] = s
    table[:, 1, :, 1] = c
    high, low = halves(table.reshape(128, 256))
    return np.concatenate([high, low, high], 1)


IN_CHUNKS = 4
OUT_CHUNKS = 8


def column_picks(y, z, gx, col):
    row = lax.broadcasted_iota(jnp.int32, (8, 32), 0)
    lane = lax.broadcasted_iota(jnp.int32, (8, 32), 1)
    block = ((col + row // 2) % 4) * 4 + gx // 16
    chosen_y = (slot_of(block, row % 2) == lane).astype(F32)
    chosen_z = (lane[:, :16] == gx % 16).astype(F32)
    y_rows = exact_dot(chosen_y, y, (1, 1))
    z_rows = exact_dot(chosen_z, z, (1, 1))
    pick = exact_dot(y_rows, repeater(8, 256, 4)) * exact_dot(z_rows, repeater(4, 256, 1))
    tall = jnp.concatenate(
        [jnp.broadcast_to(pick[n : n + 1], (8, 256)) for n in range(8)], axis=0
    )
    row = lax.broadcasted_iota(jnp.int32, (64, 256), 0)
    lane = lax.broadcasted_iota(jnp.int32, (64, 256), 1)
    return split(jnp.where(row % 8 == lane // 32, tall, 0.0))


def kept_scale(x, reach, gx, col, scale_ref):
    kz = gx % 16
    slot = lax.broadcasted_iota(jnp.int32, (32, 256), 0)
    freq = jnp.where(slot < 16, slot, 32 - slot).astype(F32)
    weight = jnp.where(kz == 0, 1.0, 2.0).astype(F32)
    block = col * 4 + gx // 16
    wide = exact_dot(x, repeater(8, 256, 1), (0, 0)) * weight
    row = lax.broadcasted_iota(jnp.int32, (16, 32), 0)
    lane = lax.broadcasted_iota(jnp.int32, (16, 32), 1)
    for member in range(2):
        here = (row == kz) & (lane == slot_of(block, member))
        bound = jnp.sum(jnp.where(here, reach.astype(F32), 0.0), axis=1, keepdims=True)
        bound = jnp.sum(bound, axis=0, keepdims=True)
        kept = jnp.where(freq < bound, wide, 0.0)
        scale_ref[member * 64 : member * 64 + 32, :] = kept[:, :128]
        scale_ref[member * 64 + 32 : member * 64 + 64, :] = kept[:, 128:]


def contract_core(core, high, low, in_rows, out_rows, sends):
    both = jnp.concatenate([high, low], axis=0)
    pad = jnp.zeros((64, 96), F32)
    for r in range(8):
        blocks = []
        for part in range(2):
            at = (part * 8 + r) * 256
            right_high, right_low = split(core[at : at + 256, :])
            out = dot(both, right_high)
            out = out[:64] + out[64:] + dot(high, right_low)
            blocks.append(jnp.concatenate([out, pad], axis=1))
        for t in range(4):
            total = blocks[0][t * 16 : t * 16 + 8]
            for part, member in ((0, 1), (1, 0), (1, 1)):
                at = t * 16 + member * 8
                total = total + pltpu.roll(
                    blocks[part][at : at + 8], 64 * part + 32 * member, 1
                )
            sends[t, r * 8 : (r + 1) * 8, :] = total
    factors = jnp.concatenate([in_rows, out_rows, jnp.zeros((16, 64), F32)], axis=1)
    for t in range(4):
        sends[t, 64:80, :] = factors


def forward_kernel(
    grid_ref, core_ref, ty_ref, tz_ref, y_ref, z_ref, x_ref, reach_ref, in_ref, out_factor_ref,
    send_ref, s0, s1, s2, s3,
    stage, core, ty, tz, y, z, x, reach, in_rows, out_rows, lines, send, sends, scale,
    arrive, small, leave,
):
    count = stage.shape[0]
    per_chunk = count // IN_CHUNKS
    gx = lax.axis_index("gx")
    col = lax.axis_index("col")

    def chunk_copy(n):
        part = pl.ds(n * per_chunk, per_chunk)
        return pltpu.make_async_copy(grid_ref.at[part], stage.at[part], arrive.at[n])

    pairs = (
        (y_ref, y), (z_ref, z), (x_ref, x), (reach_ref, reach), (in_ref, in_rows),
        (out_factor_ref, out_rows), (core_ref, core), (ty_ref, ty), (tz_ref, tz),
    )
    copies = [
        pltpu.make_async_copy(source, target, small.at[n])
        for n, (source, target) in enumerate(pairs)
    ]
    for copy in copies[:6]:
        copy.start()
    chunk_copy(0).start()
    for copy in copies[7:]:
        copy.start()
    for n in range(1, IN_CHUNKS):
        chunk_copy(n).start()
    copies[6].start()
    leaving = []
    for copy in copies[:6]:
        copy.wait()
    high, low = column_picks(y[...], z[...], gx, col)
    kept_scale(x[...], reach[...], gx, col, scale)
    copies[7].wait()
    copies[8].wait()
    table = ty[...]
    for n in range(IN_CHUNKS):
        chunk_copy(n).wait()
        for at in range(n * per_chunk, (n + 1) * per_chunk, 2):
            both = jnp.concatenate([stage[at], stage[at + 1]], axis=1)
            out = dot(table, both)
            out = out[:ROWS] + out[ROWS:]
            lines[pl.ds(at, ROWS, stride=PITCH), :] = out[:, :128]
            lines[pl.ds(at + 1, ROWS, stride=PITCH), :] = out[:, 128:]
    both_tz = tz[...]
    tz_high = both_tz[:64]
    contract = (((1,), (1,)), ((), ()))

    def piece(p):
        values = jnp.concatenate(
            [
                jnp.concatenate(
                    [lines[(at + n) * PITCH : (at + n) * PITCH + count, :] for n in range(2)], axis=0
                )
                for at in (2 * p, FREQ_ROWS + 2 * p)
            ],
            axis=1,
        )
        high, low = split(values)
        first = lax.dot_general(both_tz, high, contract, preferred_element_type=F32)
        second = lax.dot_general(tz_high, low, contract, preferred_element_type=F32)
        return first[:64] + first[64:] + second

    def ship(n):
        part = pl.ds(n * 128, 128)
        copy = pltpu.make_async_copy(send.at[part], send_ref.at[part], leave.at[5 + n])
        leaving.append(copy)
        copy.start()

    lane = lax.broadcasted_iota(jnp.int32, (32, 128), 1)
    edges = piece(0), piece(8)
    send[0:32, :] = edges[0][:32]
    send[256:288, :] = jnp.where(lane < 64, edges[1][32:], edges[0][32:])
    for p in range(1, 8):
        values = piece(p)
        send[p * 32 : (p + 1) * 32, :] = values[:32]
        send[256 + p * 32 : 256 + (p + 1) * 32, :] = values[32:]
        if p % 4 == 3:
            ship(p // 4)
            ship(2 + p // 4)
    copies[6].wait()
    contract_core(core, high, low, in_rows[...], out_rows[...], sends)
    last = [pltpu.make_async_copy(scale, s0.at[pl.ds(80, 128)], leave.at[0])]
    for t, target in enumerate((s0.at[pl.ds(0, 80)], s1, s2, s3)):
        last.append(pltpu.make_async_copy(sends.at[t], target, leave.at[1 + t]))
    for copy in last:
        copy.start()
    for copy in leaving + last:
        copy.wait()


def middle_kernel(
    got_ref, tables_ref, win_ref, scale_ref, core_ref, wout_ref, send_ref
):
    tx = table_of(tables_ref, "tx")
    lane = lax.broadcasted_iota(jnp.int32, (64, 128), 1)
    waves = []
    for pair in range(2):
        cols = [got_ref[(2 * pair + n) * 128 : (2 * pair + n + 1) * 128, :] for n in range(2)]
        high, low = split(jnp.concatenate(cols, axis=1))
        out = dot(tx, jnp.concatenate([high, high, low], axis=0))
        for n in range(2):
            part = out[:, n * 128 : (n + 1) * 128]
            picked = part[:64]
            for x in range(1, 4):
                picked = jnp.where(lane % 4 == x, part[x * 64 : (x + 1) * 64], picked)
            waves.append(picked)
    high, low = split(jnp.concatenate(waves, axis=1))
    spectrum = dot(jnp.concatenate([high, low], axis=0), table_of(tables_ref, "sum"))
    high, low = split(spectrum[:64] + spectrum[64:])
    amplitude = dot(jnp.concatenate([high, low, high], axis=1), win_ref[...])
    scale = scale_ref[...]
    scaled = amplitude * jnp.concatenate([scale, scale], axis=0)
    high, low = split(jnp.concatenate([scaled[:, :256], scaled[:, 256:]], axis=0))
    mixed = dot(jnp.concatenate([high, low, high], axis=1), core_ref[...])
    column = lane[:32] // 32 % 2
    real = jnp.where(column == 0, mixed[0:32], mixed[64:96])
    imag = jnp.where(column == 0, mixed[32:64], mixed[96:128])
    first = lane[:32] < 64
    rows = jnp.concatenate([jnp.where(first, real, imag), jnp.where(first, imag, -real)], axis=0)
    high, low = split(rows)
    contract = (((1,), (1,)), ((), ()))
    spectra = lax.dot_general(
        jnp.concatenate([high, low, high], axis=1),
        wout_ref[...],
        contract,
        preferred_element_type=F32,
    )
    high, low = split(spectra)
    both = dot(jnp.concatenate([high, low], axis=0), table_of(tables_ref, "spread"))
    vx = table_of(tables_ref, "vx")
    zero = jnp.zeros((64, 128), F32)
    for pair in range(2):
        sides = []
        for n in range(2):
            at = (2 * pair + n) * 128
            tiles = [
                [jnp.where(lane % 4 == x, values[:, at : at + 128], zero) for x in range(4)]
                for values in (both[:64], both[64:])
            ]
            sides.append(jnp.concatenate(tiles[0] + tiles[0] + tiles[1], axis=0).astype(BF16))
        out = dot(vx, jnp.concatenate(sides, axis=1))
        for n in range(2):
            at = (2 * pair + n) * 128
            send_ref[at : at + 128, :] = out[:, n * 128 : (n + 1) * 128]


@functools.cache
def sum_table():
    table = np.zeros((4, 2, 16, 4, 2, 4, 16))
    for m in range(2):
        for col in range(4):
            for c in range(16):
                table[col, m, c, :, m, col, c] = 1
    return table.reshape(512, 128).astype(ml_dtypes.bfloat16)


@functools.cache
def spread_table():
    table = np.zeros((2, 4, 16, 4, 2, 16, 4))
    for m in range(2):
        for col in range(4):
            for c in range(16):
                table[m, col, c, col, m, c, :] = 1
    return table.reshape(128, 512).astype(ml_dtypes.bfloat16)


@functools.cache
def repeat_tables():
    ranks = np.zeros((128, 32, 8))
    for r in range(32):
        ranks[r, r, :] = 1
    parts = np.zeros((2, 128, 2, 2, 32))
    for m in range(2):
        for s in range(32):
            parts[m, 32 + s, 0, m, s] = 1
            parts[m, 32 + s, 1, m, s] = -1
    table = np.concatenate(
        [ranks.reshape(128, 256), parts[0].reshape(128, 128), parts[1].reshape(128, 128)], 1
    )
    return table.astype(ml_dtypes.bfloat16)


def repeater(rows, lanes, run):
    row = lax.broadcasted_iota(jnp.int32, (rows, lanes), 0)
    lane = lax.broadcasted_iota(jnp.int32, (rows, lanes), 1)
    return (lane // run % rows == row).astype(F32)


def exact_dot(left, right, contract=(1, 0)):
    dims = (((contract[0],), (contract[1],)), ((), ()))
    return lax.dot_general(
        left, right, dims, precision=lax.Precision.HIGHEST, preferred_element_type=F32
    )


def slot_of(block, member):
    p = block - 8
    tail = jnp.where(p == 0, 16 + 15 * member, 32 - 2 * p - member)
    return jnp.where(block < 8, 2 * block + member, tail)


def own_kernel(p0, scale_ref, own_ref):
    for n in range(4):
        scale_ref[:, n * 128 : (n + 1) * 128] = p0[80 + n * 32 : 112 + n * 32, :]
    own_ref[...] = p0[:80, :]


def weights_kernel(p0, p1, p2, p3, tables_ref, win_ref, core_ref, wout_ref, tall):
    col = lax.axis_index("col")
    for t, piece in enumerate((p0, p1, p2, p3)):
        source = (col - t + 4) % 4
        high, low = split(piece[:64, :])
        at = source * 64
        core_ref[pl.ds(pl.multiple_of(at, 64), 64), :] = high
        core_ref[pl.ds(pl.multiple_of(256 + at, 64), 64), :] = high
        core_ref[pl.ds(pl.multiple_of(512 + at, 64), 64), :] = low
        tall[pl.ds(pl.multiple_of(source * 16, 16), 16), :] = piece[64:, :]
    high, low = split(tall[...])
    spread = dot(jnp.concatenate([high, low], axis=0), table_of(tables_ref, "repeat"))
    zero = jnp.zeros((64, 256), F32)
    tops = []
    for values in (spread[:64, :256], spread[64:, :256]):
        tops.append(
            jnp.concatenate(
                [jnp.concatenate([values, zero], axis=1), jnp.concatenate([zero, values], axis=1)],
                axis=0,
            ).astype(BF16)
        )
    win_ref[:128] = tops[0]
    win_ref[128:256] = tops[0]
    win_ref[256:] = tops[1]
    outs = [
        jnp.concatenate([values[:, 256:384], values[:, 384:]], axis=0).astype(BF16)
        for values in (spread[:64], spread[64:])
    ]
    wout_ref[...] = jnp.concatenate([outs[0], outs[0], outs[1]], axis=1)

def inverse_kernel(got_ref, tables_ref, out_ref, lines, stage, leave):
    count = stage.shape[0]
    per_chunk = count // OUT_CHUNKS
    for n in range(2 * FREQ_ROWS, ROWS):
        lines[n * PITCH : n * PITCH + count, :] = jnp.zeros((count, 128), F32)
    tz = [table_of(tables_ref, "tz0"), table_of(tables_ref, "tz1")]
    row = lax.broadcasted_iota(jnp.int32, (128, 128), 0)
    lane = lax.broadcasted_iota(jnp.int32, (128, 128), 1)

    def emit(p, values, pick):
        high, low = split(values)
        out = dot(jnp.concatenate([high, high, low], axis=1), tz[pick])
        for n in range(2):
            rows = out[n * count : (n + 1) * count]
            for first, values in ((2 * p, rows[:, :128]), (FREQ_ROWS + 2 * p, rows[:, 128:])):
                at = (first + n) * PITCH
                lines[at : at + count, :] = values

    for t in range(4):
        block = jnp.concatenate(
            [got_ref[t * 64 : (t + 1) * 64, :], got_ref[256 + t * 64 : 256 + (t + 1) * 64, :]],
            axis=0,
        )
        turned = block.T
        for pick in range(2):
            if t == 0 and pick == 0:
                emit(0, jnp.where((row < 64) & (lane >= 64), 0.0, turned), 0)
                emit(8, jnp.where((row < 64) & (lane >= 64), turned, 0.0), 0)
            else:
                emit(2 * t + pick, turned, pick)

    def chunk_copy(n):
        part = pl.ds(n * per_chunk, per_chunk)
        return pltpu.make_async_copy(stage.at[part], out_ref.at[part], leave.at[n])

    vy = table_of(tables_ref, "vy")
    for n in range(OUT_CHUNKS):
        for at in range(n * per_chunk, (n + 1) * per_chunk, 2):
            both = jnp.concatenate(
                [
                    lines[pl.ds(at, ROWS, stride=PITCH), :],
                    lines[pl.ds(at + 1, ROWS, stride=PITCH), :],
                ],
                axis=1,
            )
            high = both.astype(BF16).astype(F32)
            low = both - high
            rest = jnp.zeros((128 - 3 * ROWS, 256), F32)
            right = jnp.concatenate([high, high, low, rest], axis=0).astype(BF16)
            out = dot(vy, right).astype(BF16)
            stage[at] = out[:, :128]
            stage[at + 1] = out[:, 128:]
        chunk_copy(n).start()
    for n in range(OUT_CHUNKS):
        chunk_copy(n).wait()


def parts_of_tables():
    tz = z_inverse_table()
    return {
        "repeat": repeat_tables(),
        "tx": x_forward_table(),
        "sum": sum_table(),
        "spread": spread_table(),
        "vx": x_inverse_table(),
        "tz0": tz[0],
        "tz1": tz[1],
        "vy": y_inverse_table(),
    }


@functools.cache
def all_tables():
    places, blocks, at = {}, [], 0
    for name, table in parts_of_tables().items():
        places[name] = (at, *table.shape)
        for lane in range(0, table.shape[1], 128):
            blocks.append(table[:, lane : lane + 128])
            at += table.shape[0]
    return places, np.concatenate(blocks, 0)


def table_of(tables_ref, name):
    at, rows, lanes = all_tables()[0][name]
    return jnp.concatenate(
        [tables_ref[at + n * rows : at + (n + 1) * rows, :] for n in range(lanes // 128)], axis=1
    )


VMEM = pl.BlockSpec(memory_space=pltpu.VMEM)
HBM = pl.BlockSpec(memory_space=pltpu.HBM)


def room(mebibytes):
    return pltpu.CompilerParams(vmem_limit_bytes=mebibytes << 20)


def forward_call(grid_field, core, y_factor, z_factor, x_factor, kx_reach, in_factor, out_factor):
    count, grid_y, grid_z = grid_field.shape
    operands = (
        grid_field, core, y_forward_table(), z_forward_table(), y_factor.T, z_factor.T,
        x_factor.T, kx_reach.T, in_factor, out_factor,
    )
    piece = jax.ShapeDtypeStruct((80, 128), F32)
    return pl.pallas_call(
        forward_kernel,
        out_shape=(
            jax.ShapeDtypeStruct((512, 128), F32),
            jax.ShapeDtypeStruct((208, 128), F32),
            piece,
            piece,
            piece,
        ),
        in_specs=[HBM] * len(operands),
        out_specs=(HBM,) * 5,
        scratch_shapes=[pltpu.VMEM(value.shape, value.dtype) for value in operands]
        + [
            pltpu.VMEM((ROWS * PITCH, 128), F32),
            pltpu.VMEM((512, 128), F32),
            pltpu.VMEM((4, 80, 128), F32),
            pltpu.VMEM((128, 128), F32),
            pltpu.SemaphoreType.DMA((IN_CHUNKS,)),
            pltpu.SemaphoreType.DMA((9,)),
            pltpu.SemaphoreType.DMA((9,)),
        ],
        name="forward_yz",
    )(*operands)


def middle_call(got, win, scale, core, wout):
    return pl.pallas_call(
        middle_kernel,
        out_shape=jax.ShapeDtypeStruct((512, 128), F32),
        in_specs=[VMEM] * 6,
        out_specs=VMEM,
        compiler_params=room(12),
        name="mix_columns",
    )(got, all_tables()[1], win, scale, core, wout)


def own_call(piece):
    return pl.pallas_call(
        own_kernel,
        out_shape=(
            jax.ShapeDtypeStruct((32, 512), F32),
            jax.ShapeDtypeStruct((80, 128), F32),
        ),
        in_specs=[VMEM],
        out_specs=(VMEM,) * 2,
        compiler_params=room(4),
        name="own_piece",
    )(piece)


def weights_call(pieces):
    return pl.pallas_call(
        weights_kernel,
        out_shape=(
            jax.ShapeDtypeStruct((384, 512), BF16),
            jax.ShapeDtypeStruct((768, 128), BF16),
            jax.ShapeDtypeStruct((128, 384), BF16),
        ),
        in_specs=[VMEM] * 5,
        out_specs=(VMEM,) * 3,
        scratch_shapes=[pltpu.VMEM((64, 128), F32)],
        compiler_params=room(12),
        name="build_weights",
    )(*pieces, all_tables()[1])


def inverse_call(got, count, grid_y, grid_z):
    return pl.pallas_call(
        inverse_kernel,
        out_shape=jax.ShapeDtypeStruct((count, grid_y, grid_z), BF16),
        in_specs=[VMEM] * 2,
        out_specs=HBM,
        scratch_shapes=[
            pltpu.VMEM((ROWS * PITCH, 128), F32),
            pltpu.VMEM((count, grid_y, grid_z), BF16),
            pltpu.SemaphoreType.DMA((OUT_CHUNKS,)),
        ],
        compiler_params=room(16),
        name="inverse_yz",
    )(got, all_tables()[1])


def swap_over_col(pieces):
    devices = lax.axis_size("col")
    arrived = []
    for step in range(1, devices):
        ring = [(n, (n + step) % devices) for n in range(devices)]
        arrived.append(lax.ppermute(pieces[step], "col", ring))
    return arrived


def everyone(values):
    values = values.reshape(256, 2, 128)
    return lax.all_to_all(values, ("col", "gx"), 0, 0, tiled=True).reshape(512, 128)


def per_device(
    grid_field, tucker_core, in_factor, out_factor, x_factor, y_factor, z_factor, kx_reach
):
    channels, planes, grid_y, grid_z = grid_field.shape
    count = channels * planes
    core = jnp.transpose(tucker_core, (0, 1, 3, 4, 5, 2)).reshape(-1, tucker_core.shape[2])
    sent, *pieces = forward_call(
        grid_field.reshape(count, grid_y, grid_z),
        core,
        y_factor,
        z_factor,
        x_factor,
        kx_reach,
        in_factor,
        out_factor,
    )
    got = everyone(sent)
    scale, own = own_call(pieces[0])
    win, core, wout = weights_call([own] + swap_over_col(pieces))
    sent = middle_call(got, win, scale, core, wout)
    got = everyone(sent)
    result = inverse_call(got, count, grid_y, grid_z)
    return result.reshape(channels, planes, grid_y, grid_z)


def solution(mesh):
    return jax.shard_map(
        per_device,
        mesh=mesh,
        in_specs=(
            P("col", "gx", None, None),
            P(None, "col", None, None, None, None),
            P("col", None),
            P("col", None),
            P(),
            P(),
            P(),
            P(),
        ),
        out_specs=P("col", "gx", None, None),
        check_vma=False,
    )
```

```python
import functools
import math

import jax
import jax.numpy as jnp
import ml_dtypes
import numpy as np
from jax import lax
from jax.experimental import pallas as pl
from jax.experimental.pallas import tpu as pltpu
from jax.sharding import PartitionSpec as P

F32 = jnp.float32
BF16 = jnp.bfloat16
ORDER = (0, 2, 1, 3)
FREQ_ROWS = 18
ROWS = 40
PITCH = 68


def halves(table):
    table = table.astype(np.float32)
    high = table.astype(ml_dtypes.bfloat16)
    low = (table - high.astype(np.float32)).astype(ml_dtypes.bfloat16)
    return high, low


def split(values):
    high = values.astype(BF16)
    low = (values - high.astype(F32)).astype(BF16)
    return high, low


def dot(left, right):
    return jnp.dot(left, right, preferred_element_type=F32)


def dot3(left, right):
    lh, ll = split(left)
    rh, rl = split(right)
    return dot(lh, rh) + dot(lh, rl) + dot(ll, rh)


@functools.cache
def y_forward_table():
    y = np.arange(256)[None, :]
    j = np.arange(17)[:, None]
    angle = 2 * np.pi / 256 * (y * j % 256)
    table = np.zeros((ROWS, 256))
    table[:17] = np.cos(angle) / 16
    table[FREQ_ROWS : FREQ_ROWS + 17] = np.sin(angle) / 16
    high, low = halves(table)
    return np.concatenate([high, low], 0)


@functools.cache
def y_inverse_table():
    y = np.arange(256)[:, None]
    j = np.arange(17)[None, :]
    angle = 2 * np.pi / 256 * (y * j % 256)
    table = np.zeros((256, ROWS))
    table[:, :17] = np.cos(angle) / 16
    table[:, FREQ_ROWS : FREQ_ROWS + 17] = -np.sin(angle) / 16
    high, low = halves(table)
    rest = np.zeros((256, 128 - 3 * ROWS), ml_dtypes.bfloat16)
    return np.concatenate([high, low, high, rest], 1)


def z_angles():
    z = np.arange(128)[None, :]
    kz = np.arange(16)[:, None]
    angle = 2 * np.pi / 128 * (z * kz % 128)
    scale = 1 / math.sqrt(128)
    return np.cos(angle) * scale, np.sin(angle) * scale


@functools.cache
def z_forward_table():
    c, s = z_angles()
    table = np.zeros((2, 16, 2, 2, 128))
    for sign_at, sign in ((0, 1.0), (1, -1.0)):
        table[sign_at, :, 0, 0] = c
        table[sign_at, :, 0, 1] = -sign * s
        table[sign_at, :, 1, 0] = -s
        table[sign_at, :, 1, 1] = -sign * c
    high, low = halves(table.reshape(64, 256))
    return np.concatenate([high, low], 0)


@functools.cache
def z_inverse_table():
    c, s = z_angles()
    tables = []
    for pick in range(2):
        table = np.zeros((2, 2, 16, 2, 2, 128))
        for sign_at, sign in ((0, 1.0), (1, -1.0)):
            table[sign_at, pick, :, 0, 0] = c
            table[sign_at, pick, :, 1, 0] = -s
            table[sign_at, pick, :, 0, 1] = sign * s
            table[sign_at, pick, :, 1, 1] = sign * c
        high, low = halves(table.reshape(128, 256))
        tables.append(np.concatenate([high, low, high], 0))
    return np.stack(tables)


def x_angles():
    x = np.arange(256).reshape(64, 4)
    k = np.arange(32)
    freq = np.where(k < 16, k, k - 32)
    angle = 2 * np.pi / 256 * (x[:, :, None] * freq % 256)
    return np.cos(angle) / 16, np.sin(angle) / 16


@functools.cache
def x_forward_table():
    c, s = x_angles()
    table = np.zeros((4, 2, 32, 64, 2))
    table[:, 0, :, :, 0] = c.transpose(1, 2, 0)
    table[:, 0, :, :, 1] = s.transpose(1, 2, 0)
    table[:, 1, :, :, 0] = -s.transpose(1, 2, 0)
    table[:, 1, :, :, 1] = c.transpose(1, 2, 0)
    high, low = halves(table.reshape(256, 128))
    return np.concatenate([high, low, high], 1)


@functools.cache
def x_inverse_table():
    c, s = x_angles()
    table = np.zeros((64, 2, 4, 2, 32))
    table[:, 0, :, 0] = c
    table[:, 0, :, 1] = -s
    table[:, 1, :, 0] = s
    table[:, 1, :, 1] = c
    high, low = halves(table.reshape(128, 256))
    return np.concatenate([high, low, high], 1)


IN_CHUNKS = 4
OUT_CHUNKS = 8


def column_picks(y, z, gx, col):
    row = lax.broadcasted_iota(jnp.int32, (8, 32), 0)
    lane = lax.broadcasted_iota(jnp.int32, (8, 32), 1)
    block = ((col + row // 2) % 4) * 4 + gx // 16
    chosen_y = (slot_of(block, row % 2) == lane).astype(F32)
    chosen_z = (lane[:, :16] == gx % 16).astype(F32)
    y_rows = exact_dot(chosen_y, y, (1, 1))
    z_rows = exact_dot(chosen_z, z, (1, 1))
    pick = exact_dot(y_rows, repeater(8, 256, 4)) * exact_dot(z_rows, repeater(4, 256, 1))
    tall = jnp.concatenate(
        [jnp.broadcast_to(pick[n : n + 1], (8, 256)) for n in range(8)], axis=0
    )
    row = lax.broadcasted_iota(jnp.int32, (64, 256), 0)
    lane = lax.broadcasted_iota(jnp.int32, (64, 256), 1)
    return split(jnp.where(row % 8 == lane // 32, tall, 0.0))


def kept_scale(x, reach, gx, col, scale_ref):
    kz = gx % 16
    slot = lax.broadcasted_iota(jnp.int32, (32, 256), 0)
    freq = jnp.where(slot < 16, slot, 32 - slot).astype(F32)
    weight = jnp.where(kz == 0, 1.0, 2.0).astype(F32)
    block = col * 4 + gx // 16
    wide = exact_dot(x, repeater(8, 256, 1), (0, 0)) * weight
    row = lax.broadcasted_iota(jnp.int32, (16, 32), 0)
    lane = lax.broadcasted_iota(jnp.int32, (16, 32), 1)
    for member in range(2):
        here = (row == kz) & (lane == slot_of(block, member))
        bound = jnp.sum(jnp.where(here, reach.astype(F32), 0.0), axis=1, keepdims=True)
        bound = jnp.sum(bound, axis=0, keepdims=True)
        kept = jnp.where(freq < bound, wide, 0.0)
        scale_ref[member * 64 : member * 64 + 32, :] = kept[:, :128]
        scale_ref[member * 64 + 32 : member * 64 + 64, :] = kept[:, 128:]


def contract_core(core, high, low, in_rows, out_rows, sends):
    both = jnp.concatenate([high, low], axis=0)
    pad = jnp.zeros((64, 96), F32)
    for r in range(8):
        blocks = []
        for part in range(2):
            at = (part * 8 + r) * 256
            right_high, right_low = split(core[at : at + 256, :])
            out = dot(both, right_high)
            out = out[:64] + out[64:] + dot(high, right_low)
            blocks.append(jnp.concatenate([out, pad], axis=1))
        for t in range(4):
            total = blocks[0][t * 16 : t * 16 + 8]
            for part, member in ((0, 1), (1, 0), (1, 1)):
                at = t * 16 + member * 8
                total = total + pltpu.roll(
                    blocks[part][at : at + 8], 64 * part + 32 * member, 1
                )
            sends[t, r * 8 : (r + 1) * 8, :] = total
    factors = jnp.concatenate([in_rows, out_rows, jnp.zeros((16, 64), F32)], axis=1)
    for t in range(4):
        sends[t, 64:80, :] = factors


def forward_kernel(
    grid_ref, core_ref, ty_ref, tz_ref, y_ref, z_ref, x_ref, reach_ref, in_ref, out_factor_ref,
    send_ref, s0, s1, s2, s3,
    stage, core, ty, tz, y, z, x, reach, in_rows, out_rows, lines, send, sends, scale,
    arrive, small, leave,
):
    count = stage.shape[0]
    per_chunk = count // IN_CHUNKS
    gx = lax.axis_index("gx")
    col = lax.axis_index("col")

    def chunk_copy(n):
        part = pl.ds(n * per_chunk, per_chunk)
        return pltpu.make_async_copy(grid_ref.at[part], stage.at[part], arrive.at[n])

    pairs = (
        (y_ref, y), (z_ref, z), (x_ref, x), (reach_ref, reach), (in_ref, in_rows),
        (out_factor_ref, out_rows), (core_ref, core), (ty_ref, ty), (tz_ref, tz),
    )
    copies = [
        pltpu.make_async_copy(source, target, small.at[n])
        for n, (source, target) in enumerate(pairs)
    ]
    for copy in copies[:6]:
        copy.start()
    chunk_copy(0).start()
    for copy in copies[7:]:
        copy.start()
    for n in range(1, IN_CHUNKS):
        chunk_copy(n).start()
    copies[6].start()
    leaving = []
    for copy in copies[:6]:
        copy.wait()
    high, low = column_picks(y[...], z[...], gx, col)
    kept_scale(x[...], reach[...], gx, col, scale)
    copies[7].wait()
    copies[8].wait()
    table = ty[...]
    for n in range(IN_CHUNKS):
        chunk_copy(n).wait()
        for at in range(n * per_chunk, (n + 1) * per_chunk, 2):
            both = jnp.concatenate([stage[at], stage[at + 1]], axis=1)
            out = dot(table, both)
            out = out[:ROWS] + out[ROWS:]
            lines[pl.ds(at, ROWS, stride=PITCH), :] = out[:, :128]
            lines[pl.ds(at + 1, ROWS, stride=PITCH), :] = out[:, 128:]
    both_tz = tz[...]
    tz_high = both_tz[:64]
    contract = (((1,), (1,)), ((), ()))

    def piece(p):
        values = jnp.concatenate(
            [
                jnp.concatenate(
                    [lines[(at + n) * PITCH : (at + n) * PITCH + count, :] for n in range(2)], axis=0
                )
                for at in (2 * p, FREQ_ROWS + 2 * p)
            ],
            axis=1,
        )
        high, low = split(values)
        first = lax.dot_general(both_tz, high, contract, preferred_element_type=F32)
        second = lax.dot_general(tz_high, low, contract, preferred_element_type=F32)
        return first[:64] + first[64:] + second

    def ship(n):
        part = pl.ds(n * 128, 128)
        copy = pltpu.make_async_copy(send.at[part], send_ref.at[part], leave.at[5 + n])
        leaving.append(copy)
        copy.start()

    lane = lax.broadcasted_iota(jnp.int32, (32, 128), 1)
    edges = piece(0), piece(8)
    send[0:32, :] = edges[0][:32]
    send[256:288, :] = jnp.where(lane < 64, edges[1][32:], edges[0][32:])
    for p in range(1, 8):
        values = piece(p)
        send[p * 32 : (p + 1) * 32, :] = values[:32]
        send[256 + p * 32 : 256 + (p + 1) * 32, :] = values[32:]
        if p % 4 == 3:
            ship(p // 4)
            ship(2 + p // 4)
    copies[6].wait()
    contract_core(core, high, low, in_rows[...], out_rows[...], sends)
    last = [pltpu.make_async_copy(scale, s0.at[pl.ds(80, 128)], leave.at[0])]
    for t, target in zip(ORDER, (s0.at[pl.ds(0, 80)], s1, s2, s3)):
        last.append(pltpu.make_async_copy(sends.at[t], target, leave.at[1 + t]))
    for copy in last:
        copy.start()
    for copy in leaving + last:
        copy.wait()


def middle_kernel(
    got_ref, tables_ref, win_ref, scale_ref, core_ref, wout_ref, send_ref
):
    tx = table_of(tables_ref, "tx")
    lane = lax.broadcasted_iota(jnp.int32, (64, 128), 1)
    waves = []
    for pair in range(2):
        cols = [got_ref[(2 * pair + n) * 128 : (2 * pair + n + 1) * 128, :] for n in range(2)]
        high, low = split(jnp.concatenate(cols, axis=1))
        out = dot(tx, jnp.concatenate([high, high, low], axis=0))
        for n in range(2):
            part = out[:, n * 128 : (n + 1) * 128]
            picked = part[:64]
            for x in range(1, 4):
                picked = jnp.where(lane % 4 == x, part[x * 64 : (x + 1) * 64], picked)
            waves.append(picked)
    high, low = split(jnp.concatenate(waves, axis=1))
    spectrum = dot(jnp.concatenate([high, low], axis=0), table_of(tables_ref, "sum"))
    high, low = split(spectrum[:64] + spectrum[64:])
    amplitude = dot(jnp.concatenate([high, low, high], axis=1), win_ref[...])
    scale = scale_ref[...]
    scaled = amplitude * jnp.concatenate([scale, scale], axis=0)
    high, low = split(jnp.concatenate([scaled[:, :256], scaled[:, 256:]], axis=0))
    mixed = dot(jnp.concatenate([high, low, high], axis=1), core_ref[...])
    column = lane[:32] // 32 % 2
    real = jnp.where(column == 0, mixed[0:32], mixed[64:96])
    imag = jnp.where(column == 0, mixed[32:64], mixed[96:128])
    first = lane[:32] < 64
    rows = jnp.concatenate([jnp.where(first, real, imag), jnp.where(first, imag, -real)], axis=0)
    high, low = split(rows)
    contract = (((1,), (1,)), ((), ()))
    spectra = lax.dot_general(
        jnp.concatenate([high, low, high], axis=1),
        wout_ref[...],
        contract,
        preferred_element_type=F32,
    )
    high, low = split(spectra)
    both = dot(jnp.concatenate([high, low], axis=0), table_of(tables_ref, "spread"))
    vx = table_of(tables_ref, "vx")
    zero = jnp.zeros((64, 128), F32)
    for pair in range(2):
        sides = []
        for n in range(2):
            at = (2 * pair + n) * 128
            tiles = [
                [jnp.where(lane % 4 == x, values[:, at : at + 128], zero) for x in range(4)]
                for values in (both[:64], both[64:])
            ]
            sides.append(jnp.concatenate(tiles[0] + tiles[0] + tiles[1], axis=0).astype(BF16))
        out = dot(vx, jnp.concatenate(sides, axis=1))
        for n in range(2):
            at = (2 * pair + n) * 128
            send_ref[at : at + 128, :] = out[:, n * 128 : (n + 1) * 128]


@functools.cache
def sum_table():
    table = np.zeros((4, 2, 16, 4, 2, 4, 16))
    for m in range(2):
        for col in range(4):
            for c in range(16):
                table[col, m, c, :, m, col, c] = 1
    return table.reshape(512, 128).astype(ml_dtypes.bfloat16)


@functools.cache
def spread_table():
    table = np.zeros((2, 4, 16, 4, 2, 16, 4))
    for m in range(2):
        for col in range(4):
            for c in range(16):
                table[m, col, c, col, m, c, :] = 1
    return table.reshape(128, 512).astype(ml_dtypes.bfloat16)


@functools.cache
def repeat_tables():
    ranks = np.zeros((128, 32, 8))
    for r in range(32):
        ranks[r, r, :] = 1
    parts = np.zeros((2, 128, 2, 2, 32))
    for m in range(2):
        for s in range(32):
            parts[m, 32 + s, 0, m, s] = 1
            parts[m, 32 + s, 1, m, s] = -1
    table = np.concatenate(
        [ranks.reshape(128, 256), parts[0].reshape(128, 128), parts[1].reshape(128, 128)], 1
    )
    return table.astype(ml_dtypes.bfloat16)


def repeater(rows, lanes, run):
    row = lax.broadcasted_iota(jnp.int32, (rows, lanes), 0)
    lane = lax.broadcasted_iota(jnp.int32, (rows, lanes), 1)
    return (lane // run % rows == row).astype(F32)


def exact_dot(left, right, contract=(1, 0)):
    dims = (((contract[0],), (contract[1],)), ((), ()))
    return lax.dot_general(
        left, right, dims, precision=lax.Precision.HIGHEST, preferred_element_type=F32
    )


def slot_of(block, member):
    p = block - 8
    tail = jnp.where(p == 0, 16 + 15 * member, 32 - 2 * p - member)
    return jnp.where(block < 8, 2 * block + member, tail)


def own_kernel(p0, scale_ref, own_ref):
    for n in range(4):
        scale_ref[:, n * 128 : (n + 1) * 128] = p0[80 + n * 32 : 112 + n * 32, :]
    own_ref[...] = p0[:80, :]


def weights_kernel(p0, p1, p2, p3, tables_ref, win_ref, core_ref, wout_ref, tall):
    col = lax.axis_index("col")
    for t, piece in zip(ORDER, (p0, p1, p2, p3)):
        source = (col - t + 4) % 4
        high, low = split(piece[:64, :])
        at = source * 64
        core_ref[pl.ds(pl.multiple_of(at, 64), 64), :] = high
        core_ref[pl.ds(pl.multiple_of(256 + at, 64), 64), :] = high
        core_ref[pl.ds(pl.multiple_of(512 + at, 64), 64), :] = low
        tall[pl.ds(pl.multiple_of(source * 16, 16), 16), :] = piece[64:, :]
    high, low = split(tall[...])
    spread = dot(jnp.concatenate([high, low], axis=0), table_of(tables_ref, "repeat"))
    zero = jnp.zeros((64, 256), F32)
    tops = []
    for values in (spread[:64, :256], spread[64:, :256]):
        tops.append(
            jnp.concatenate(
                [jnp.concatenate([values, zero], axis=1), jnp.concatenate([zero, values], axis=1)],
                axis=0,
            ).astype(BF16)
        )
    win_ref[:128] = tops[0]
    win_ref[128:256] = tops[0]
    win_ref[256:] = tops[1]
    outs = [
        jnp.concatenate([values[:, 256:384], values[:, 384:]], axis=0).astype(BF16)
        for values in (spread[:64], spread[64:])
    ]
    wout_ref[...] = jnp.concatenate([outs[0], outs[0], outs[1]], axis=1)

def inverse_kernel(got_ref, tables_ref, out_ref, lines, stage, leave):
    count = stage.shape[0]
    per_chunk = count // OUT_CHUNKS
    for n in range(2 * FREQ_ROWS, ROWS):
        lines[n * PITCH : n * PITCH + count, :] = jnp.zeros((count, 128), F32)
    tz = [table_of(tables_ref, "tz0"), table_of(tables_ref, "tz1")]
    row = lax.broadcasted_iota(jnp.int32, (128, 128), 0)
    lane = lax.broadcasted_iota(jnp.int32, (128, 128), 1)

    def emit(p, values, pick):
        high, low = split(values)
        out = dot(jnp.concatenate([high, high, low], axis=1), tz[pick])
        for n in range(2):
            rows = out[n * count : (n + 1) * count]
            for first, values in ((2 * p, rows[:, :128]), (FREQ_ROWS + 2 * p, rows[:, 128:])):
                at = (first + n) * PITCH
                lines[at : at + count, :] = values

    for t in range(4):
        block = jnp.concatenate(
            [got_ref[t * 64 : (t + 1) * 64, :], got_ref[256 + t * 64 : 256 + (t + 1) * 64, :]],
            axis=0,
        )
        turned = block.T
        for pick in range(2):
            if t == 0 and pick == 0:
                emit(0, jnp.where((row < 64) & (lane >= 64), 0.0, turned), 0)
                emit(8, jnp.where((row < 64) & (lane >= 64), turned, 0.0), 0)
            else:
                emit(2 * t + pick, turned, pick)

    def chunk_copy(n):
        part = pl.ds(n * per_chunk, per_chunk)
        return pltpu.make_async_copy(stage.at[part], out_ref.at[part], leave.at[n])

    vy = table_of(tables_ref, "vy")
    for n in range(OUT_CHUNKS):
        for at in range(n * per_chunk, (n + 1) * per_chunk, 2):
            both = jnp.concatenate(
                [
                    lines[pl.ds(at, ROWS, stride=PITCH), :],
                    lines[pl.ds(at + 1, ROWS, stride=PITCH), :],
                ],
                axis=1,
            )
            high = both.astype(BF16).astype(F32)
            low = both - high
            rest = jnp.zeros((128 - 3 * ROWS, 256), F32)
            right = jnp.concatenate([high, high, low, rest], axis=0).astype(BF16)
            out = dot(vy, right).astype(BF16)
            stage[at] = out[:, :128]
            stage[at + 1] = out[:, 128:]
        chunk_copy(n).start()
    for n in range(OUT_CHUNKS):
        chunk_copy(n).wait()


def parts_of_tables():
    tz = z_inverse_table()
    return {
        "repeat": repeat_tables(),
        "tx": x_forward_table(),
        "sum": sum_table(),
        "spread": spread_table(),
        "vx": x_inverse_table(),
        "tz0": tz[0],
        "tz1": tz[1],
        "vy": y_inverse_table(),
    }


@functools.cache
def all_tables():
    places, blocks, at = {}, [], 0
    for name, table in parts_of_tables().items():
        places[name] = (at, *table.shape)
        for lane in range(0, table.shape[1], 128):
            blocks.append(table[:, lane : lane + 128])
            at += table.shape[0]
    return places, np.concatenate(blocks, 0)


def table_of(tables_ref, name):
    at, rows, lanes = all_tables()[0][name]
    return jnp.concatenate(
        [tables_ref[at + n * rows : at + (n + 1) * rows, :] for n in range(lanes // 128)], axis=1
    )


VMEM = pl.BlockSpec(memory_space=pltpu.VMEM)
HBM = pl.BlockSpec(memory_space=pltpu.HBM)


def room(mebibytes):
    return pltpu.CompilerParams(vmem_limit_bytes=mebibytes << 20)


def forward_call(grid_field, core, y_factor, z_factor, x_factor, kx_reach, in_factor, out_factor):
    count, grid_y, grid_z = grid_field.shape
    operands = (
        grid_field, core, y_forward_table(), z_forward_table(), y_factor.T, z_factor.T,
        x_factor.T, kx_reach.T, in_factor, out_factor,
    )
    piece = jax.ShapeDtypeStruct((80, 128), F32)
    return pl.pallas_call(
        forward_kernel,
        out_shape=(
            jax.ShapeDtypeStruct((512, 128), F32),
            jax.ShapeDtypeStruct((208, 128), F32),
            piece,
            piece,
            piece,
        ),
        in_specs=[HBM] * len(operands),
        out_specs=(HBM,) * 5,
        scratch_shapes=[pltpu.VMEM(value.shape, value.dtype) for value in operands]
        + [
            pltpu.VMEM((ROWS * PITCH, 128), F32),
            pltpu.VMEM((512, 128), F32),
            pltpu.VMEM((4, 80, 128), F32),
            pltpu.VMEM((128, 128), F32),
            pltpu.SemaphoreType.DMA((IN_CHUNKS,)),
            pltpu.SemaphoreType.DMA((9,)),
            pltpu.SemaphoreType.DMA((9,)),
        ],
        name="forward_yz",
    )(*operands)


def middle_call(got, win, scale, core, wout):
    return pl.pallas_call(
        middle_kernel,
        out_shape=jax.ShapeDtypeStruct((512, 128), F32),
        in_specs=[VMEM] * 6,
        out_specs=VMEM,
        compiler_params=room(12),
        name="mix_columns",
    )(got, all_tables()[1], win, scale, core, wout)


def own_call(piece):
    return pl.pallas_call(
        own_kernel,
        out_shape=(
            jax.ShapeDtypeStruct((32, 512), F32),
            jax.ShapeDtypeStruct((80, 128), F32),
        ),
        in_specs=[VMEM],
        out_specs=(VMEM,) * 2,
        compiler_params=room(4),
        name="own_piece",
    )(piece)


def weights_call(pieces):
    return pl.pallas_call(
        weights_kernel,
        out_shape=(
            jax.ShapeDtypeStruct((384, 512), BF16),
            jax.ShapeDtypeStruct((768, 128), BF16),
            jax.ShapeDtypeStruct((128, 384), BF16),
        ),
        in_specs=[VMEM] * 5,
        out_specs=(VMEM,) * 3,
        scratch_shapes=[pltpu.VMEM((64, 128), F32)],
        compiler_params=room(12),
        name="build_weights",
    )(*pieces, all_tables()[1])


def inverse_call(got, count, grid_y, grid_z):
    return pl.pallas_call(
        inverse_kernel,
        out_shape=jax.ShapeDtypeStruct((count, grid_y, grid_z), BF16),
        in_specs=[VMEM] * 2,
        out_specs=HBM,
        scratch_shapes=[
            pltpu.VMEM((ROWS * PITCH, 128), F32),
            pltpu.VMEM((count, grid_y, grid_z), BF16),
            pltpu.SemaphoreType.DMA((OUT_CHUNKS,)),
        ],
        compiler_params=room(16),
        name="inverse_yz",
    )(got, all_tables()[1])


def swap_over_col(pieces):
    devices = lax.axis_size("col")
    arrived = []
    for step, piece in zip(ORDER[1:], pieces[1:]):
        ring = [(n, (n + step) % devices) for n in range(devices)]
        arrived.append(lax.ppermute(piece, "col", ring))
    return arrived


def everyone(values):
    values = values.reshape(256, 2, 128)
    return lax.all_to_all(values, ("col", "gx"), 0, 0, tiled=True).reshape(512, 128)


def per_device(
    grid_field, tucker_core, in_factor, out_factor, x_factor, y_factor, z_factor, kx_reach
):
    channels, planes, grid_y, grid_z = grid_field.shape
    count = channels * planes
    core = jnp.transpose(tucker_core, (0, 1, 3, 4, 5, 2)).reshape(-1, tucker_core.shape[2])
    sent, *pieces = forward_call(
        grid_field.reshape(count, grid_y, grid_z),
        core,
        y_factor,
        z_factor,
        x_factor,
        kx_reach,
        in_factor,
        out_factor,
    )
    got = everyone(sent)
    scale, own = own_call(pieces[0])
    win, core, wout = weights_call([own] + swap_over_col(pieces))
    sent = middle_call(got, win, scale, core, wout)
    got = everyone(sent)
    result = inverse_call(got, count, grid_y, grid_z)
    return result.reshape(channels, planes, grid_y, grid_z)


def solution(mesh):
    return jax.shard_map(
        per_device,
        mesh=mesh,
        in_specs=(
            P("col", "gx", None, None),
            P(None, "col", None, None, None, None),
            P("col", None),
            P("col", None),
            P(),
            P(),
            P(),
            P(),
        ),
        out_specs=P("col", "gx", None, None),
        check_vma=False,
    )
```

```python
import functools
import math

import jax
import jax.numpy as jnp
import ml_dtypes
import numpy as np
from jax import lax
from jax.experimental import pallas as pl
from jax.experimental.pallas import tpu as pltpu
from jax.sharding import PartitionSpec as P

F32 = jnp.float32
BF16 = jnp.bfloat16
ORDER = (0, 1, 3, 2)
FREQ_ROWS = 18
ROWS = 40
PITCH = 68


def halves(table):
    table = table.astype(np.float32)
    high = table.astype(ml_dtypes.bfloat16)
    low = (table - high.astype(np.float32)).astype(ml_dtypes.bfloat16)
    return high, low


def split(values):
    high = values.astype(BF16)
    low = (values - high.astype(F32)).astype(BF16)
    return high, low


def dot(left, right):
    return jnp.dot(left, right, preferred_element_type=F32)


def dot3(left, right):
    lh, ll = split(left)
    rh, rl = split(right)
    return dot(lh, rh) + dot(lh, rl) + dot(ll, rh)


@functools.cache
def y_forward_table():
    y = np.arange(256)[None, :]
    j = np.arange(17)[:, None]
    angle = 2 * np.pi / 256 * (y * j % 256)
    table = np.zeros((ROWS, 256))
    table[:17] = np.cos(angle) / 16
    table[FREQ_ROWS : FREQ_ROWS + 17] = np.sin(angle) / 16
    high, low = halves(table)
    return np.concatenate([high, low], 0)


@functools.cache
def y_inverse_table():
    y = np.arange(256)[:, None]
    j = np.arange(17)[None, :]
    angle = 2 * np.pi / 256 * (y * j % 256)
    table = np.zeros((256, ROWS))
    table[:, :17] = np.cos(angle) / 16
    table[:, FREQ_ROWS : FREQ_ROWS + 17] = -np.sin(angle) / 16
    high, low = halves(table)
    rest = np.zeros((256, 128 - 3 * ROWS), ml_dtypes.bfloat16)
    return np.concatenate([high, low, high, rest], 1)


def z_angles():
    z = np.arange(128)[None, :]
    kz = np.arange(16)[:, None]
    angle = 2 * np.pi / 128 * (z * kz % 128)
    scale = 1 / math.sqrt(128)
    return np.cos(angle) * scale, np.sin(angle) * scale


@functools.cache
def z_forward_table():
    c, s = z_angles()
    table = np.zeros((2, 16, 2, 2, 128))
    for sign_at, sign in ((0, 1.0), (1, -1.0)):
        table[sign_at, :, 0, 0] = c
        table[sign_at, :, 0, 1] = -sign * s
        table[sign_at, :, 1, 0] = -s
        table[sign_at, :, 1, 1] = -sign * c
    high, low = halves(table.reshape(64, 256))
    return np.concatenate([high, low], 0)


@functools.cache
def z_inverse_table():
    c, s = z_angles()
    tables = []
    for pick in range(2):
        table = np.zeros((2, 2, 16, 2, 2, 128))
        for sign_at, sign in ((0, 1.0), (1, -1.0)):
            table[sign_at, pick, :, 0, 0] = c
            table[sign_at, pick, :, 1, 0] = -s
            table[sign_at, pick, :, 0, 1] = sign * s
            table[sign_at, pick, :, 1, 1] = sign * c
        high, low = halves(table.reshape(128, 256))
        tables.append(np.concatenate([high, low, high], 0))
    return np.stack(tables)


def x_angles():
    x = np.arange(256).reshape(64, 4)
    k = np.arange(32)
    freq = np.where(k < 16, k, k - 32)
    angle = 2 * np.pi / 256 * (x[:, :, None] * freq % 256)
    return np.cos(angle) / 16, np.sin(angle) / 16


@functools.cache
def x_forward_table():
    c, s = x_angles()
    table = np.zeros((4, 2, 32, 64, 2))
    table[:, 0, :, :, 0] = c.transpose(1, 2, 0)
    table[:, 0, :, :, 1] = s.transpose(1, 2, 0)
    table[:, 1, :, :, 0] = -s.transpose(1, 2, 0)
    table[:, 1, :, :, 1] = c.transpose(1, 2, 0)
    high, low = halves(table.reshape(256, 128))
    return np.concatenate([high, low, high], 1)


@functools.cache
def x_inverse_table():
    c, s = x_angles()
    table = np.zeros((64, 2, 4, 2, 32))
    table[:, 0, :, 0] = c
    table[:, 0, :, 1] = -s
    table[:, 1, :, 0] = s
    table[:, 1, :, 1] = c
    high, low = halves(table.reshape(128, 256))
    return np.concatenate([high, low, high], 1)


IN_CHUNKS = 4
OUT_CHUNKS = 8


def column_picks(y, z, gx, col):
    row = lax.broadcasted_iota(jnp.int32, (8, 32), 0)
    lane = lax.broadcasted_iota(jnp.int32, (8, 32), 1)
    block = ((col + row // 2) % 4) * 4 + gx // 16
    chosen_y = (slot_of(block, row % 2) == lane).astype(F32)
    chosen_z = (lane[:, :16] == gx % 16).astype(F32)
    y_rows = exact_dot(chosen_y, y, (1, 1))
    z_rows = exact_dot(chosen_z, z, (1, 1))
    pick = exact_dot(y_rows, repeater(8, 256, 4)) * exact_dot(z_rows, repeater(4, 256, 1))
    tall = jnp.concatenate(
        [jnp.broadcast_to(pick[n : n + 1], (8, 256)) for n in range(8)], axis=0
    )
    row = lax.broadcasted_iota(jnp.int32, (64, 256), 0)
    lane = lax.broadcasted_iota(jnp.int32, (64, 256), 1)
    return split(jnp.where(row % 8 == lane // 32, tall, 0.0))


def kept_scale(x, reach, gx, col, scale_ref):
    kz = gx % 16
    slot = lax.broadcasted_iota(jnp.int32, (32, 256), 0)
    freq = jnp.where(slot < 16, slot, 32 - slot).astype(F32)
    weight = jnp.where(kz == 0, 1.0, 2.0).astype(F32)
    block = col * 4 + gx // 16
    wide = exact_dot(x, repeater(8, 256, 1), (0, 0)) * weight
    row = lax.broadcasted_iota(jnp.int32, (16, 32), 0)
    lane = lax.broadcasted_iota(jnp.int32, (16, 32), 1)
    for member in range(2):
        here = (row == kz) & (lane == slot_of(block, member))
        bound = jnp.sum(jnp.where(here, reach.astype(F32), 0.0), axis=1, keepdims=True)
        bound = jnp.sum(bound, axis=0, keepdims=True)
        kept = jnp.where(freq < bound, wide, 0.0)
        scale_ref[member * 64 : member * 64 + 32, :] = kept[:, :128]
        scale_ref[member * 64 + 32 : member * 64 + 64, :] = kept[:, 128:]


def contract_core(core, high, low, in_rows, out_rows, sends):
    both = jnp.concatenate([high, low], axis=0)
    pad = jnp.zeros((64, 96), F32)
    for r in range(8):
        blocks = []
        for part in range(2):
            at = (part * 8 + r) * 256
            right_high, right_low = split(core[at : at + 256, :])
            out = dot(both, right_high)
            out = out[:64] + out[64:] + dot(high, right_low)
            blocks.append(jnp.concatenate([out, pad], axis=1))
        for t in range(4):
            total = blocks[0][t * 16 : t * 16 + 8]
            for part, member in ((0, 1), (1, 0), (1, 1)):
                at = t * 16 + member * 8
                total = total + pltpu.roll(
                    blocks[part][at : at + 8], 64 * part + 32 * member, 1
                )
            sends[t, r * 8 : (r + 1) * 8, :] = total
    factors = jnp.concatenate([in_rows, out_rows, jnp.zeros((16, 64), F32)], axis=1)
    for t in range(4):
        sends[t, 64:80, :] = factors


def forward_kernel(
    grid_ref, core_ref, ty_ref, tz_ref, y_ref, z_ref, x_ref, reach_ref, in_ref, out_factor_ref,
    send_ref, s0, s1, s2, s3,
    stage, core, ty, tz, y, z, x, reach, in_rows, out_rows, lines, send, sends, scale,
    arrive, small, leave,
):
    count = stage.shape[0]
    per_chunk = count // IN_CHUNKS
    gx = lax.axis_index("gx")
    col = lax.axis_index("col")

    def chunk_copy(n):
        part = pl.ds(n * per_chunk, per_chunk)
        return pltpu.make_async_copy(grid_ref.at[part], stage.at[part], arrive.at[n])

    pairs = (
        (y_ref, y), (z_ref, z), (x_ref, x), (reach_ref, reach), (in_ref, in_rows),
        (out_factor_ref, out_rows), (core_ref, core), (ty_ref, ty), (tz_ref, tz),
    )
    copies = [
        pltpu.make_async_copy(source, target, small.at[n])
        for n, (source, target) in enumerate(pairs)
    ]
    for copy in copies[:6]:
        copy.start()
    chunk_copy(0).start()
    for copy in copies[7:]:
        copy.start()
    for n in range(1, IN_CHUNKS):
        chunk_copy(n).start()
    copies[6].start()
    leaving = []
    for copy in copies[:6]:
        copy.wait()
    high, low = column_picks(y[...], z[...], gx, col)
    kept_scale(x[...], reach[...], gx, col, scale)
    copies[7].wait()
    copies[8].wait()
    table = ty[...]
    for n in range(IN_CHUNKS):
        chunk_copy(n).wait()
        for at in range(n * per_chunk, (n + 1) * per_chunk, 2):
            both = jnp.concatenate([stage[at], stage[at + 1]], axis=1)
            out = dot(table, both)
            out = out[:ROWS] + out[ROWS:]
            lines[pl.ds(at, ROWS, stride=PITCH), :] = out[:, :128]
            lines[pl.ds(at + 1, ROWS, stride=PITCH), :] = out[:, 128:]
    both_tz = tz[...]
    tz_high = both_tz[:64]
    contract = (((1,), (1,)), ((), ()))

    def piece(p):
        values = jnp.concatenate(
            [
                jnp.concatenate(
                    [lines[(at + n) * PITCH : (at + n) * PITCH + count, :] for n in range(2)], axis=0
                )
                for at in (2 * p, FREQ_ROWS + 2 * p)
            ],
            axis=1,
        )
        high, low = split(values)
        first = lax.dot_general(both_tz, high, contract, preferred_element_type=F32)
        second = lax.dot_general(tz_high, low, contract, preferred_element_type=F32)
        return first[:64] + first[64:] + second

    def ship(n):
        part = pl.ds(n * 128, 128)
        copy = pltpu.make_async_copy(send.at[part], send_ref.at[part], leave.at[5 + n])
        leaving.append(copy)
        copy.start()

    lane = lax.broadcasted_iota(jnp.int32, (32, 128), 1)
    edges = piece(0), piece(8)
    send[0:32, :] = edges[0][:32]
    send[256:288, :] = jnp.where(lane < 64, edges[1][32:], edges[0][32:])
    for p in range(1, 8):
        values = piece(p)
        send[p * 32 : (p + 1) * 32, :] = values[:32]
        send[256 + p * 32 : 256 + (p + 1) * 32, :] = values[32:]
        if p % 4 == 3:
            ship(p // 4)
            ship(2 + p // 4)
    copies[6].wait()
    contract_core(core, high, low, in_rows[...], out_rows[...], sends)
    last = [pltpu.make_async_copy(scale, s0.at[pl.ds(80, 128)], leave.at[0])]
    for t, target in zip(ORDER, (s0.at[pl.ds(0, 80)], s1, s2, s3)):
        last.append(pltpu.make_async_copy(sends.at[t], target, leave.at[1 + t]))
    for copy in last:
        copy.start()
    for copy in leaving + last:
        copy.wait()


def middle_kernel(
    got_ref, tables_ref, win_ref, scale_ref, core_ref, wout_ref, send_ref
):
    tx = table_of(tables_ref, "tx")
    lane = lax.broadcasted_iota(jnp.int32, (64, 128), 1)
    waves = []
    for pair in range(2):
        cols = [got_ref[(2 * pair + n) * 128 : (2 * pair + n + 1) * 128, :] for n in range(2)]
        high, low = split(jnp.concatenate(cols, axis=1))
        out = dot(tx, jnp.concatenate([high, high, low], axis=0))
        for n in range(2):
            part = out[:, n * 128 : (n + 1) * 128]
            picked = part[:64]
            for x in range(1, 4):
                picked = jnp.where(lane % 4 == x, part[x * 64 : (x + 1) * 64], picked)
            waves.append(picked)
    high, low = split(jnp.concatenate(waves, axis=1))
    spectrum = dot(jnp.concatenate([high, low], axis=0), table_of(tables_ref, "sum"))
    high, low = split(spectrum[:64] + spectrum[64:])
    amplitude = dot(jnp.concatenate([high, low, high], axis=1), win_ref[...])
    scale = scale_ref[...]
    scaled = amplitude * jnp.concatenate([scale, scale], axis=0)
    high, low = split(jnp.concatenate([scaled[:, :256], scaled[:, 256:]], axis=0))
    mixed = dot(jnp.concatenate([high, low, high], axis=1), core_ref[...])
    column = lane[:32] // 32 % 2
    real = jnp.where(column == 0, mixed[0:32], mixed[64:96])
    imag = jnp.where(column == 0, mixed[32:64], mixed[96:128])
    first = lane[:32] < 64
    rows = jnp.concatenate([jnp.where(first, real, imag), jnp.where(first, imag, -real)], axis=0)
    high, low = split(rows)
    contract = (((1,), (1,)), ((), ()))
    spectra = lax.dot_general(
        jnp.concatenate([high, low, high], axis=1),
        wout_ref[...],
        contract,
        preferred_element_type=F32,
    )
    high, low = split(spectra)
    both = dot(jnp.concatenate([high, low], axis=0), table_of(tables_ref, "spread"))
    vx = table_of(tables_ref, "vx")
    zero = jnp.zeros((64, 128), F32)
    for pair in range(2):
        sides = []
        for n in range(2):
            at = (2 * pair + n) * 128
            tiles = [
                [jnp.where(lane % 4 == x, values[:, at : at + 128], zero) for x in range(4)]
                for values in (both[:64], both[64:])
            ]
            sides.append(jnp.concatenate(tiles[0] + tiles[0] + tiles[1], axis=0).astype(BF16))
        out = dot(vx, jnp.concatenate(sides, axis=1))
        for n in range(2):
            at = (2 * pair + n) * 128
            send_ref[at : at + 128, :] = out[:, n * 128 : (n + 1) * 128]


@functools.cache
def sum_table():
    table = np.zeros((4, 2, 16, 4, 2, 4, 16))
    for m in range(2):
        for col in range(4):
            for c in range(16):
                table[col, m, c, :, m, col, c] = 1
    return table.reshape(512, 128).astype(ml_dtypes.bfloat16)


@functools.cache
def spread_table():
    table = np.zeros((2, 4, 16, 4, 2, 16, 4))
    for m in range(2):
        for col in range(4):
            for c in range(16):
                table[m, col, c, col, m, c, :] = 1
    return table.reshape(128, 512).astype(ml_dtypes.bfloat16)


@functools.cache
def repeat_tables():
    ranks = np.zeros((128, 32, 8))
    for r in range(32):
        ranks[r, r, :] = 1
    parts = np.zeros((2, 128, 2, 2, 32))
    for m in range(2):
        for s in range(32):
            parts[m, 32 + s, 0, m, s] = 1
            parts[m, 32 + s, 1, m, s] = -1
    table = np.concatenate(
        [ranks.reshape(128, 256), parts[0].reshape(128, 128), parts[1].reshape(128, 128)], 1
    )
    return table.astype(ml_dtypes.bfloat16)


def repeater(rows, lanes, run):
    row = lax.broadcasted_iota(jnp.int32, (rows, lanes), 0)
    lane = lax.broadcasted_iota(jnp.int32, (rows, lanes), 1)
    return (lane // run % rows == row).astype(F32)


def exact_dot(left, right, contract=(1, 0)):
    dims = (((contract[0],), (contract[1],)), ((), ()))
    return lax.dot_general(
        left, right, dims, precision=lax.Precision.HIGHEST, preferred_element_type=F32
    )


def slot_of(block, member):
    p = block - 8
    tail = jnp.where(p == 0, 16 + 15 * member, 32 - 2 * p - member)
    return jnp.where(block < 8, 2 * block + member, tail)


def own_kernel(p0, scale_ref, own_ref):
    for n in range(4):
        scale_ref[:, n * 128 : (n + 1) * 128] = p0[80 + n * 32 : 112 + n * 32, :]
    own_ref[...] = p0[:80, :]


def weights_kernel(p0, p1, p2, p3, tables_ref, win_ref, core_ref, wout_ref, tall):
    col = lax.axis_index("col")
    for t, piece in zip(ORDER, (p0, p1, p2, p3)):
        source = (col - t + 4) % 4
        high, low = split(piece[:64, :])
        at = source * 64
        core_ref[pl.ds(pl.multiple_of(at, 64), 64), :] = high
        core_ref[pl.ds(pl.multiple_of(256 + at, 64), 64), :] = high
        core_ref[pl.ds(pl.multiple_of(512 + at, 64), 64), :] = low
        tall[pl.ds(pl.multiple_of(source * 16, 16), 16), :] = piece[64:, :]
    high, low = split(tall[...])
    spread = dot(jnp.concatenate([high, low], axis=0), table_of(tables_ref, "repeat"))
    zero = jnp.zeros((64, 256), F32)
    tops = []
    for values in (spread[:64, :256], spread[64:, :256]):
        tops.append(
            jnp.concatenate(
                [jnp.concatenate([values, zero], axis=1), jnp.concatenate([zero, values], axis=1)],
                axis=0,
            ).astype(BF16)
        )
    win_ref[:128] = tops[0]
    win_ref[128:256] = tops[0]
    win_ref[256:] = tops[1]
    outs = [
        jnp.concatenate([values[:, 256:384], values[:, 384:]], axis=0).astype(BF16)
        for values in (spread[:64], spread[64:])
    ]
    wout_ref[...] = jnp.concatenate([outs[0], outs[0], outs[1]], axis=1)

def inverse_kernel(got_ref, tables_ref, out_ref, lines, stage, leave):
    count = stage.shape[0]
    per_chunk = count // OUT_CHUNKS
    for n in range(2 * FREQ_ROWS, ROWS):
        lines[n * PITCH : n * PITCH + count, :] = jnp.zeros((count, 128), F32)
    tz = [table_of(tables_ref, "tz0"), table_of(tables_ref, "tz1")]
    row = lax.broadcasted_iota(jnp.int32, (128, 128), 0)
    lane = lax.broadcasted_iota(jnp.int32, (128, 128), 1)

    def emit(p, values, pick):
        high, low = split(values)
        out = dot(jnp.concatenate([high, high, low], axis=1), tz[pick])
        for n in range(2):
            rows = out[n * count : (n + 1) * count]
            for first, values in ((2 * p, rows[:, :128]), (FREQ_ROWS + 2 * p, rows[:, 128:])):
                at = (first + n) * PITCH
                lines[at : at + count, :] = values

    for t in range(4):
        block = jnp.concatenate(
            [got_ref[t * 64 : (t + 1) * 64, :], got_ref[256 + t * 64 : 256 + (t + 1) * 64, :]],
            axis=0,
        )
        turned = block.T
        for pick in range(2):
            if t == 0 and pick == 0:
                emit(0, jnp.where((row < 64) & (lane >= 64), 0.0, turned), 0)
                emit(8, jnp.where((row < 64) & (lane >= 64), turned, 0.0), 0)
            else:
                emit(2 * t + pick, turned, pick)

    def chunk_copy(n):
        part = pl.ds(n * per_chunk, per_chunk)
        return pltpu.make_async_copy(stage.at[part], out_ref.at[part], leave.at[n])

    vy = table_of(tables_ref, "vy")
    for n in range(OUT_CHUNKS):
        for at in range(n * per_chunk, (n + 1) * per_chunk, 2):
            both = jnp.concatenate(
                [
                    lines[pl.ds(at, ROWS, stride=PITCH), :],
                    lines[pl.ds(at + 1, ROWS, stride=PITCH), :],
                ],
                axis=1,
            )
            high = both.astype(BF16).astype(F32)
            low = both - high
            rest = jnp.zeros((128 - 3 * ROWS, 256), F32)
            right = jnp.concatenate([high, high, low, rest], axis=0).astype(BF16)
            out = dot(vy, right).astype(BF16)
            stage[at] = out[:, :128]
            stage[at + 1] = out[:, 128:]
        chunk_copy(n).start()
    for n in range(OUT_CHUNKS):
        chunk_copy(n).wait()


def parts_of_tables():
    tz = z_inverse_table()
    return {
        "repeat": repeat_tables(),
        "tx": x_forward_table(),
        "sum": sum_table(),
        "spread": spread_table(),
        "vx": x_inverse_table(),
        "tz0": tz[0],
        "tz1": tz[1],
        "vy": y_inverse_table(),
    }


@functools.cache
def all_tables():
    places, blocks, at = {}, [], 0
    for name, table in parts_of_tables().items():
        places[name] = (at, *table.shape)
        for lane in range(0, table.shape[1], 128):
            blocks.append(table[:, lane : lane + 128])
            at += table.shape[0]
    return places, np.concatenate(blocks, 0)


def table_of(tables_ref, name):
    at, rows, lanes = all_tables()[0][name]
    return jnp.concatenate(
        [tables_ref[at + n * rows : at + (n + 1) * rows, :] for n in range(lanes // 128)], axis=1
    )


VMEM = pl.BlockSpec(memory_space=pltpu.VMEM)
HBM = pl.BlockSpec(memory_space=pltpu.HBM)


def room(mebibytes):
    return pltpu.CompilerParams(vmem_limit_bytes=mebibytes << 20)


def forward_call(grid_field, core, y_factor, z_factor, x_factor, kx_reach, in_factor, out_factor):
    count, grid_y, grid_z = grid_field.shape
    operands = (
        grid_field, core, y_forward_table(), z_forward_table(), y_factor.T, z_factor.T,
        x_factor.T, kx_reach.T, in_factor, out_factor,
    )
    piece = jax.ShapeDtypeStruct((80, 128), F32)
    return pl.pallas_call(
        forward_kernel,
        out_shape=(
            jax.ShapeDtypeStruct((512, 128), F32),
            jax.ShapeDtypeStruct((208, 128), F32),
            piece,
            piece,
            piece,
        ),
        in_specs=[HBM] * len(operands),
        out_specs=(HBM,) * 5,
        scratch_shapes=[pltpu.VMEM(value.shape, value.dtype) for value in operands]
        + [
            pltpu.VMEM((ROWS * PITCH, 128), F32),
            pltpu.VMEM((512, 128), F32),
            pltpu.VMEM((4, 80, 128), F32),
            pltpu.VMEM((128, 128), F32),
            pltpu.SemaphoreType.DMA((IN_CHUNKS,)),
            pltpu.SemaphoreType.DMA((9,)),
            pltpu.SemaphoreType.DMA((9,)),
        ],
        name="forward_yz",
    )(*operands)


def middle_call(got, win, scale, core, wout):
    return pl.pallas_call(
        middle_kernel,
        out_shape=jax.ShapeDtypeStruct((512, 128), F32),
        in_specs=[VMEM] * 6,
        out_specs=VMEM,
        compiler_params=room(12),
        name="mix_columns",
    )(got, all_tables()[1], win, scale, core, wout)


def own_call(piece):
    return pl.pallas_call(
        own_kernel,
        out_shape=(
            jax.ShapeDtypeStruct((32, 512), F32),
            jax.ShapeDtypeStruct((80, 128), F32),
        ),
        in_specs=[VMEM],
        out_specs=(VMEM,) * 2,
        compiler_params=room(4),
        name="own_piece",
    )(piece)


def weights_call(pieces):
    return pl.pallas_call(
        weights_kernel,
        out_shape=(
            jax.ShapeDtypeStruct((384, 512), BF16),
            jax.ShapeDtypeStruct((768, 128), BF16),
            jax.ShapeDtypeStruct((128, 384), BF16),
        ),
        in_specs=[VMEM] * 5,
        out_specs=(VMEM,) * 3,
        scratch_shapes=[pltpu.VMEM((64, 128), F32)],
        compiler_params=room(12),
        name="build_weights",
    )(*pieces, all_tables()[1])


def inverse_call(got, count, grid_y, grid_z):
    return pl.pallas_call(
        inverse_kernel,
        out_shape=jax.ShapeDtypeStruct((count, grid_y, grid_z), BF16),
        in_specs=[VMEM] * 2,
        out_specs=HBM,
        scratch_shapes=[
            pltpu.VMEM((ROWS * PITCH, 128), F32),
            pltpu.VMEM((count, grid_y, grid_z), BF16),
            pltpu.SemaphoreType.DMA((OUT_CHUNKS,)),
        ],
        compiler_params=room(16),
        name="inverse_yz",
    )(got, all_tables()[1])


def swap_over_col(pieces):
    devices = lax.axis_size("col")
    arrived = []
    for step, piece in zip(ORDER[1:], pieces[1:]):
        ring = [(n, (n + step) % devices) for n in range(devices)]
        arrived.append(lax.ppermute(piece, "col", ring))
    return arrived


def everyone(values):
    values = values.reshape(256, 2, 128)
    return lax.all_to_all(values, ("col", "gx"), 0, 0, tiled=True).reshape(512, 128)


def per_device(
    grid_field, tucker_core, in_factor, out_factor, x_factor, y_factor, z_factor, kx_reach
):
    channels, planes, grid_y, grid_z = grid_field.shape
    count = channels * planes
    core = jnp.transpose(tucker_core, (0, 1, 3, 4, 5, 2)).reshape(-1, tucker_core.shape[2])
    sent, *pieces = forward_call(
        grid_field.reshape(count, grid_y, grid_z),
        core,
        y_factor,
        z_factor,
        x_factor,
        kx_reach,
        in_factor,
        out_factor,
    )
    got = everyone(sent)
    scale, own = own_call(pieces[0])
    win, core, wout = weights_call([own] + swap_over_col(pieces))
    sent = middle_call(got, win, scale, core, wout)
    got = everyone(sent)
    result = inverse_call(got, count, grid_y, grid_z)
    return result.reshape(channels, planes, grid_y, grid_z)


def solution(mesh):
    return jax.shard_map(
        per_device,
        mesh=mesh,
        in_specs=(
            P("col", "gx", None, None),
            P(None, "col", None, None, None, None),
            P("col", None),
            P("col", None),
            P(),
            P(),
            P(),
            P(),
        ),
        out_specs=P("col", "gx", None, None),
        check_vma=False,
    )
```
